128 devices in a mesh: prow: 8 (over y, core), pcol: 16 (over z, x).
Axes of the slice: x: 4, y: 4, z: 4, core: 2. Of those that a mesh axis runs over, the one named last changes fastest.
Arguments:
- inverse_cov: bfloat16 [8192, 8192], P('prow', 'pcol'), may hold values from -0.5 to 4.5, as said below
- cosines: float32 [8192, 8192], P('prow', 'pcol'), may hold values from -1 to 1, as said below
- sky_maps: bfloat16 [8192, 192], P('pcol'), may hold values from -6 to 6
Outputs:
- filtered: bfloat16 [8192, 192], P('prow')
- spectra: float32 [64, 192], replicated
The draws below stay inside these ranges and needn't reach their ends.
Inputs may be any that keep to these rules, and one draw needn't show every extreme that they name: `inverse_cov`: symmetric, with a dominant diagonal. `cosines`: symmetric.
All inputs are finite; a program needn't handle non-finite values.
Results may differ from the reference program's by a relative error of at most 0.0033.
Values may be sent and summed in bfloat16 or wider, within the bound.
A program may use at most 64 MiB of HBM per device.

```python
import math
import jax
import jax.numpy as jnp
from jax import lax

NPIX = 8192
MAPS = 192
L = 64
LMIN = 2


def draw_inverse_cov(key, part):
    first_key, second_key = jax.random.split(jax.random.fold_in(key, 11))
    noise = jax.random.truncated_normal(first_key, -6.0, 6.0, (NPIX, NPIX), jnp.float32) * (0.5 / math.sqrt(NPIX))
    symmetric = noise + noise.T
    diagonal = jax.random.uniform(second_key, (NPIX,), jnp.float32, 1.0, 2.0)
    return (symmetric + jnp.diag(diagonal)).astype(jnp.bfloat16)


def draw_cosines(key, part):
    vector_key, rough_key = jax.random.split(jax.random.fold_in(key, 23))
    vectors = jax.random.normal(vector_key, (NPIX, 3), jnp.float32)
    rough = jax.random.truncated_normal(rough_key, -4.0, 4.0, (NPIX, NPIX), jnp.float32) * 0.05
    units = vectors / jnp.sqrt(jnp.sum(vectors * vectors, axis=1, keepdims=True) + 1e-12)
    product = jnp.dot(units, units.T, precision=lax.Precision.HIGHEST)
    return jnp.clip(product + rough + rough.T, -1.0, 1.0)


def shard_levels(rng, extent, pieces, smallest, high):
    level = 1.0
    for dim, shards_of in pieces:
        steps = jax.random.uniform(jax.random.fold_in(jax.random.fold_in(rng, 6), dim), (shards_of,), jnp.float32, smallest / len(pieces), high / len(pieces))
        level = level * jnp.repeat(jnp.exp(steps), extent[dim] // shards_of).reshape((-1,) + (1,) * (len(extent) - 1 - dim))
    return level


def normal_values(rng, shape, scale, limit, cuts=(), kind=jnp.bfloat16):
    values = scale * jax.random.normal(rng, shape, jnp.float32)
    if cuts:
        values = values * shard_levels(rng, shape, cuts, -0.22, 0.18)
    return jnp.clip(values, -limit, limit).astype(kind)


def setup_inputs(seed: int = 0) -> dict:
    streams_of = jax.random.split(jax.random.key(seed), 4)
    inverse_cov = draw_inverse_cov(jax.random.fold_in(streams_of[3], 71), 0)
    cosines = draw_cosines(jax.random.fold_in(streams_of[3], 71), 0)
    sky_maps = normal_values(streams_of[2], (NPIX, MAPS), 1.0, 6.0, ((0, 16),))
    return {"inverse_cov": inverse_cov, "cosines": cosines, "sky_maps": sky_maps}


def next_legendre(previous, current, cosine, degree):
    return ((2.0 * degree - 1.0) * cosine * current - (degree - 1.0) * previous) / degree


def reference(inverse_cov, cosines, sky_maps):
    filtered = jnp.dot(inverse_cov, sky_maps, preferred_element_type=jnp.float32).astype(jnp.bfloat16)
    maps_f32 = filtered.astype(jnp.float32)
    blocks = 8
    size_rows = NPIX // blocks
    degrees = (jnp.arange(L) + LMIN).astype(jnp.float32)

    def block_spectra(block_index):
        first_row = (block_index * size_rows).astype(jnp.int32)
        cosine = lax.dynamic_slice_in_dim(cosines, first_row, size_rows, 0)
        rows_f32 = lax.dynamic_slice_in_dim(maps_f32, first_row, size_rows, 0)
        previous = jnp.ones_like(cosine)
        current = cosine
        for low_degree in range(2, LMIN):
            next_term = next_legendre(previous, current, cosine, jnp.float32(low_degree))
            previous, current = current, next_term

        def advance(carried, degree):
            previous, current = carried
            next_term = next_legendre(previous, current, cosine, degree)
            product = jnp.dot(next_term.astype(jnp.bfloat16), filtered, preferred_element_type=jnp.float32)
            spectrum = jnp.sum(rows_f32 * product, axis=0) * ((2.0 * degree + 1.0) / NPIX)
            return (current, next_term), spectrum

        carried, values = lax.scan(advance, (previous, current), degrees)
        return values

    per_block = lax.map(block_spectra, jnp.arange(blocks, dtype=jnp.int32))
    return filtered, jnp.sum(per_block, axis=0)
```

```python
import functools
import math
import random

import jax
import jax.numpy as jnp
import numpy as np
from jax import lax
from jax.experimental import pallas as pl
from jax.experimental.pallas import tpu as pltpu
from jax.sharding import PartitionSpec as P

L = 64
LMIN = 2
TILE = 256
STRIP = 16
GROUP = 11
CHUNKS = 6
LEVELS = GROUP * CHUNKS


def transform_matrix(npix, devices):
    top = LMIN + L - 1
    each = -(-L // devices)
    a = [math.comb(2 * k, k) / 4.0**k for k in range(top + 1)]
    out = np.zeros((devices * each, LEVELS))
    for l in range(LMIN, top + 1):
        owner, place = divmod(l - LMIN, each)
        row = out[owner * each + place]
        for k in range(l + 1):
            row[abs(l - 2 * k)] += a[k] * a[l - k]
        row *= (2 * l + 1) / npix
    return out.astype(np.float32), each


def pair_up(tiles, n):
    items = []
    for col in range(n):
        mine = sorted((t for t in tiles if t[1] == col), key=lambda t: t[0])
        for k in range(0, len(mine), 2):
            first = mine[k]
            second = mine[k + 1] if k + 1 < len(mine) else (first[0], col, 0)
            items.append((first[0], second[0], first[2], second[2], col))
    return items


def work_tables(n):
    lower = [[(h * n + i, j, 2) for i in range(n) for j in range(n)] for h in range(2)]
    rng = random.Random(0)
    best = None
    for _ in range(20000):
        sets = []
        cross = [[rng.random() < 0.5 for _ in range(n)] for _ in range(n)]
        for h in range(2):
            tiles = []
            for i in range(n):
                tiles.append((h * n + i, i, 1))
                for j in range(i):
                    a, b = (i, j) if rng.random() < 0.5 else (j, i)
                    tiles.append((h * n + a, b, 2))
                for j in range(n):
                    if h == 0 and cross[i][j]:
                        tiles.append((n + i, j, 2))
                    if h == 1 and not cross[i][j]:
                        tiles.append((j, i, 2))
            sets.append(pair_up(tiles, n))
        cost = max(len(s) for s in sets)
        if best is None or cost < best[0]:
            best = (cost, sets)
        if 2 * cost <= n * n + n // 2 + 1:
            break
    kinds = [pair_up(lower[0], n), pair_up(lower[1], n), pair_up(lower[1], n), pair_up(lower[0], n)] + best[1]
    longest = max(len(k) for k in kinds)
    table = np.zeros((len(kinds), longest + 1, 5), np.int32)
    for k, items in enumerate(kinds):
        table[k, : len(items)] = items
    counts = np.array([len(k) for k in kinds], np.int32)
    return table.reshape(-1), counts, longest + 1


def moments_kernel(
    stride, table, counts, cos_hbm, ft, fct, out,
    xbuf, x2, prev, cur, buf_a, buf_b, lhs, fj, acc, sem,
):
    r = lax.axis_index("prow")
    c = lax.axis_index("pcol")
    q, h = c // 2, c % 2
    kind = jnp.where(r > q, h, jnp.where(r < q, 2 + h, 4 + h))
    n_items = counts[kind]

    def field(item, f):
        return table[(kind * stride + item) * 5 + f]

    def tile_copy(item, half):
        row = pl.multiple_of(field(item, half) * TILE, TILE)
        col = pl.multiple_of(field(item, 4) * TILE, TILE)
        return pltpu.make_async_copy(
            cos_hbm.at[pl.ds(row, TILE), pl.ds(col, TILE)],
            xbuf.at[pl.ds(half * TILE, TILE)],
            sem.at[half],
        )

    def fetch(item):
        tile_copy(item, 0).start()
        tile_copy(item, 1).start()

    def begin(item):
        tile_copy(item, 0).wait()
        tile_copy(item, 1).wait()
        x = xbuf[...]
        x2[...] = x + x
        prev[...] = (x + x) * x - 1.0
        cur[...] = x

    def set_operands(item):
        col = pl.multiple_of(field(item, 4) * TILE, TILE)
        for half in range(2):
            row = pl.multiple_of(field(item, half) * TILE, TILE)
            weight = field(item, 2 + half).astype(jnp.float32)
            value = ft[:, pl.ds(row, TILE)].astype(jnp.float32) * weight
            lhs[:, half * TILE : (half + 1) * TILE] = value.astype(jnp.bfloat16)
        fj[...] = fct[:, pl.ds(col, TILE)].astype(jnp.float32)

    n_strips = 2 * TILE // STRIP

    def gen_strip(buf, s):
        rows = pl.ds(s * STRIP, STRIP)
        xx = x2[rows, :]
        p = prev[rows, :]
        t = cur[rows, :]
        for g in range(GROUP):
            p, t = t, xx * t - p
            buf[g, rows, :] = t.astype(jnp.bfloat16)
        prev[rows, :] = p
        cur[rows, :] = t

    def half_step(gen, use, level0):
        done = 0
        for g in range(GROUP):
            upto = (g + 1) * n_strips // GROUP
            for s in range(done, upto):
                gen_strip(gen, s)
            done = upto
            image = jnp.dot(lhs[...], use[g], preferred_element_type=jnp.float32)
            prod = image * fj[...]
            half_tile = TILE // 2
            acc[level0 + g] += prod[:, :half_tile] + prod[:, half_tile:]

    acc[...] = jnp.zeros_like(acc)
    fetch(0)
    begin(0)
    for s in range(n_strips):
        gen_strip(buf_a, s)

    def item_loop(item, carry):
        fetch(item + 1)
        set_operands(item)

        def chunk_loop(cp, carry):
            half_step(buf_b, buf_a, cp * 2 * GROUP)

            @pl.when(cp == CHUNKS // 2 - 1)
            def _():
                begin(item + 1)

            half_step(buf_a, buf_b, cp * 2 * GROUP + GROUP)
            return carry

        return lax.fori_loop(0, CHUNKS // 2, chunk_loop, carry)

    lax.fori_loop(0, n_items, item_loop, 0)
    out[...] = jnp.sum(acc[...], axis=-1)


def spectra_moments(cosines, ft, fct):
    maps = ft.shape[0]
    n = cosines.shape[1] // TILE
    table, counts, stride = work_tables(n)
    vmem = pl.BlockSpec(memory_space=pltpu.VMEM)
    smem = pl.BlockSpec(memory_space=pltpu.SMEM)
    return pl.pallas_call(
        functools.partial(moments_kernel, stride),
        out_shape=jax.ShapeDtypeStruct((LEVELS, maps), jnp.float32),
        in_specs=[smem, smem, pl.BlockSpec(memory_space=pl.ANY), vmem, vmem],
        out_specs=vmem,
        scratch_shapes=[
            pltpu.VMEM((2 * TILE, TILE), jnp.float32),
            pltpu.VMEM((2 * TILE, TILE), jnp.float32),
            pltpu.VMEM((2 * TILE, TILE), jnp.float32),
            pltpu.VMEM((2 * TILE, TILE), jnp.float32),
            pltpu.VMEM((GROUP, 2 * TILE, TILE), jnp.bfloat16),
            pltpu.VMEM((GROUP, 2 * TILE, TILE), jnp.bfloat16),
            pltpu.VMEM((maps, 2 * TILE), jnp.bfloat16),
            pltpu.VMEM((maps, TILE), jnp.float32),
            pltpu.VMEM((LEVELS, maps, TILE // 2), jnp.float32),
            pltpu.SemaphoreType.DMA((2,)),
        ],
        compiler_params=pltpu.CompilerParams(vmem_limit_bytes=48 * 2**20),
        name="moments",
    )(jnp.asarray(table), jnp.asarray(counts), cosines, ft, fct)


MESH = pl.DeviceIdType.MESH


def rank_order(rows, cols):
    spots = [(dz, dx) for dz in range(rows) for dx in range(cols) if dz or dx]
    reach = lambda d, n: min(d, n - d)
    return sorted(spots, key=lambda s: -(reach(s[0], rows) + reach(s[1], cols)))


def filter_kernel(
    n_rows, n_z, n_x, sky, cov, rows_out, cols_out, part, parcel, landed, mine,
    send1, recv1, send2, recv2, send3, recv3,
):
    r = lax.axis_index("prow")
    c = lax.axis_index("pcol")
    n = n_z * n_x
    z, x = c // n_x, lax.rem(c, n_x)
    half_n = n // 2
    maps = sky.shape[1]
    per, width = parcel.shape[1], parcel.shape[2]
    barrier = pltpu.get_barrier_semaphore()
    order = rank_order(n_z, n_x)
    home = c // 2
    from_other = r != home

    def peer(spot):
        return lax.rem(z + spot[0], n_z) * n_x + lax.rem(x + spot[1], n_x)

    def peer_back(spot):
        return lax.rem(z - spot[0] + n_z, n_z) * n_x + lax.rem(x - spot[1] + n_x, n_x)

    def signal(device):
        pl.semaphore_signal(barrier, inc=1, device_id=device, device_id_type=MESH)

    for spot in order:
        signal((r, peer(spot)))

    @pl.when(from_other)
    def _():
        for j in range(half_n):
            signal((home, lax.rem(c, 2) * half_n + j))

    sky_t = sky[...].astype(jnp.float32).T.astype(jnp.bfloat16)
    wide = 2 * width
    for g in range(cov.shape[0] // wide):
        value = lax.dot_general(
            sky_t, cov[g * wide : (g + 1) * wide, :], (((1,), (1,)), ((), ())),
            preferred_element_type=jnp.float32,
        )
        for a in range(2):
            for b in range(maps // per):
                k = (2 * g + a) * (maps // per) + b
                piece = value[b * per : (b + 1) * per, a * width : (a + 1) * width]
                part[k] = piece
                parcel[k] = piece.astype(jnp.bfloat16)

    pl.semaphore_wait(barrier, len(order) + n_rows - 1)

    def copy(src, dst, send, recv, device):
        return pltpu.make_async_remote_copy(
            src_ref=src, dst_ref=dst, send_sem=send, recv_sem=recv,
            device_id=device, device_id_type=MESH,
        )

    def scatter(s):
        to = peer(order[s])
        return copy(parcel.at[to], landed.at[s], send1.at[s], recv1.at[s], (r, to))

    for s in range(len(order)):
        scatter(s).start()
    total = part[c]
    for s in range(len(order)):
        scatter(s).wait_recv()
        total = total + landed[s].astype(jnp.float32)
    mine[...] = total.astype(jnp.bfloat16)

    def row_place(k):
        return rows_out.at[
            pl.ds(pl.multiple_of(lax.rem(k, 2) * per, per), per),
            pl.ds(pl.multiple_of((k // 2) * width, width), width),
        ]

    def col_place(k):
        return cols_out.at[
            pl.ds(pl.multiple_of(lax.rem(k, 2) * per, per), per),
            pl.ds(pl.multiple_of((lax.rem(k, half_n) // 2) * width, width), width),
        ]

    def gather(s, k):
        return copy(mine, row_place(k), send2.at[s], recv2.at[s], (r, peer(order[s])))

    def column(e):
        return copy(
            mine, col_place(c), send3.at[e - 1], recv3.at[lax.rem(c, half_n)],
            (lax.rem(r + e, n_rows), 2 * r + c // half_n),
        )

    far = [4, 5, 3, 2, 6, 1, 7]
    for s in range(8):
        gather(s, c).start()
    for e in far:
        column(e).start()
    for s in range(8, len(order)):
        gather(s, c).start()
    rows_out[
        pl.ds(pl.multiple_of(lax.rem(c, 2) * per, per), per),
        pl.ds(pl.multiple_of((c // 2) * width, width), width),
    ] = mine[...]

    for s in range(len(order)):
        gather(s, peer_back(order[s])).wait_recv()

    @pl.when(from_other)
    def _():
        for j in range(half_n):
            copy(
                mine, col_place(j), send3.at[0], recv3.at[j],
                (home, lax.rem(c, 2) * half_n + j),
            ).wait_recv()

    @pl.when(jnp.logical_not(from_other))
    def _():
        size = cols_out.shape[1]
        cols_out[...] = rows_out[:, pl.ds(pl.multiple_of(lax.rem(c, 2) * size, size), size)]

    for s in range(len(order)):
        scatter(s).wait_send()
        gather(s, c).wait_send()
    for e in far:
        column(e).wait_send()


def filter_maps(sky, cov, n_rows, n_z, n_x, collective_id):
    n = n_z * n_x
    maps, size = sky.shape[1], cov.shape[0]
    per, width = maps // 2, 2 * size // n
    vmem = pl.BlockSpec(memory_space=pltpu.VMEM)
    plane = pltpu.SemaphoreType.DMA((n - 1,))
    return pl.pallas_call(
        functools.partial(filter_kernel, n_rows, n_z, n_x),
        out_shape=(
            jax.ShapeDtypeStruct((maps, size), jnp.bfloat16),
            jax.ShapeDtypeStruct((maps, cov.shape[1]), jnp.bfloat16),
        ),
        in_specs=[vmem, vmem],
        out_specs=(vmem, vmem),
        scratch_shapes=[
            pltpu.VMEM((n, per, width), jnp.float32),
            pltpu.VMEM((n, per, width), jnp.bfloat16),
            pltpu.VMEM((n - 1, per, width), jnp.bfloat16),
            pltpu.VMEM((per, width), jnp.bfloat16),
            plane, plane, plane, plane,
            pltpu.SemaphoreType.DMA((n_rows - 1,)),
            pltpu.SemaphoreType.DMA((n // 2,)),
        ],
        compiler_params=pltpu.CompilerParams(
            collective_id=collective_id, has_side_effects=True
        ),
        name="filter",
    )(sky, cov)


def total_kernel(
    n_rows, n_z, n_x, x, out, landed, mine, others, result,
    send1, recv1, send2, recv2, send3, recv3,
):
    r = lax.axis_index("prow")
    c = lax.axis_index("pcol")
    z, xx = c // n_x, lax.rem(c, n_x)
    order = rank_order(n_z, n_x)
    per = x.shape[0] // n_rows
    barrier = pltpu.get_barrier_semaphore()
    far = [4, 5, 3, 2, 6, 1, 7]

    def peer(spot):
        return lax.rem(z + spot[0], n_z) * n_x + lax.rem(xx + spot[1], n_x)

    def line(e):
        return lax.rem(r + e, n_rows)

    def signal(device):
        pl.semaphore_signal(barrier, inc=1, device_id=device, device_id_type=MESH)

    for spot in order:
        signal((r, peer(spot)))
    for e in far:
        signal((line(e), c))
    pl.semaphore_wait(barrier, len(order) + len(far))

    def block(k):
        return pl.ds(pl.multiple_of(k * per, per), per)

    def copy(src, dst, send, recv, device):
        return pltpu.make_async_remote_copy(
            src_ref=src, dst_ref=dst, send_sem=send, recv_sem=recv,
            device_id=device, device_id_type=MESH,
        )

    def first(e):
        return copy(x.at[block(line(e))], landed.at[e - 1], send1.at[e - 1], recv1.at[e - 1], (line(e), c))

    def second(s):
        return copy(mine, others.at[c], send2.at[s], recv2.at[s], (r, peer(order[s])))

    def third(e, k):
        return copy(result, out.at[block(k)], send3.at[e - 1], recv3.at[e - 1], (line(e), c))

    for e in far:
        first(e).start()
    total = x[block(r)]
    for e in far:
        first(e).wait_recv()
    for e in range(1, n_rows):
        total = total + landed[e - 1]
    mine[...] = total
    for s in range(len(order)):
        second(s).start()
    others[c] = total
    for s in range(len(order)):
        second(s).wait_recv()
    total = others[0]
    for k in range(1, n_z * n_x):
        total = total + others[k]
    result[...] = total
    for e in far:
        third(e, r).start()
    out[block(r)] = total
    for e in far:
        third(e, lax.rem(r - e + n_rows, n_rows)).wait_recv()
    for e in far:
        first(e).wait_send()
        third(e, r).wait_send()
    for s in range(len(order)):
        second(s).wait_send()


def total_over_all(x, n_rows, n_z, n_x, collective_id):
    n = n_z * n_x
    per, cols = x.shape[0] // n_rows, x.shape[1]
    vmem = pl.BlockSpec(memory_space=pltpu.VMEM)
    plane = pltpu.SemaphoreType.DMA((n - 1,))
    line = pltpu.SemaphoreType.DMA((n_rows - 1,))
    return pl.pallas_call(
        functools.partial(total_kernel, n_rows, n_z, n_x),
        out_shape=jax.ShapeDtypeStruct(x.shape, x.dtype),
        in_specs=[vmem],
        out_specs=vmem,
        scratch_shapes=[
            pltpu.VMEM((n_rows - 1, per, cols), x.dtype),
            pltpu.VMEM((per, cols), x.dtype),
            pltpu.VMEM((n, per, cols), x.dtype),
            pltpu.VMEM((per, cols), x.dtype),
            line, line, plane, plane, line, line,
        ],
        compiler_params=pltpu.CompilerParams(
            collective_id=collective_id, has_side_effects=True
        ),
        name="total",
    )(x)


N_X = 4


def per_device(npix, n_rows, n_cols, inverse_cov, cosines, sky_maps):
    n_z = n_cols // N_X
    row_maps, column_maps = filter_maps(sky_maps, inverse_cov, n_rows, n_z, N_X, 1)
    moments = spectra_moments(cosines, row_maps, column_maps)
    matrix, _ = transform_matrix(npix, 1)
    partial_spectra = jnp.dot(jnp.asarray(matrix), moments, precision=lax.Precision.HIGHEST)
    spectra = total_over_all(partial_spectra, n_rows, n_z, N_X, 2)
    return (row_maps.T, spectra)


def solution(mesh):
    in_specs = (P("prow", "pcol"), P("prow", "pcol"), P("pcol", None))
    out_specs = (P("prow", None), P())
    n_rows, n_cols = mesh.shape["prow"], mesh.shape["pcol"]

    def whole(inverse_cov, cosines, sky_maps):
        npix = cosines.shape[0]
        step = jax.shard_map(
            functools.partial(per_device, npix, n_rows, n_cols),
            mesh=mesh, in_specs=in_specs, out_specs=out_specs, check_vma=False,
        )
        return step(inverse_cov, cosines, sky_maps)

    return whole
```

```python
import functools
import math

import jax
import jax.numpy as jnp
import numpy as np
from jax import lax
from jax.experimental import pallas as pl
from jax.experimental.pallas import tpu as pltpu
from jax.sharding import PartitionSpec as P

L = 64
LMIN = 2
TOP = LMIN + L - 1
LEVELS = TOP + 1
UNROLL = 6
TILE = 256
STRIP = 32
N_X = 4
LANES = 128
MESH = pl.DeviceIdType.MESH


def transform_matrix(npix):
    a = [math.comb(2 * k, k) / 4.0**k for k in range(TOP + 1)]
    out = np.zeros((-(-LEVELS // 8) * 8, LANES))
    for l in range(LMIN, TOP + 1):
        for k in range(l + 1):
            out[abs(l - 2 * k), l - LMIN] += a[k] * a[l - k] * (2 * l + 1) / npix
    return out.astype(np.float32)


def rank_order(rows, cols):
    spots = [(dz, dx) for dz in range(rows) for dx in range(cols) if dz or dx]
    reach = lambda d, n: min(d, n - d)
    return sorted(spots, key=lambda s: -(reach(s[0], rows) + reach(s[1], cols)))


LINE = [4, 5, 3, 2, 6, 1, 7]


def qml_kernel(
    n_rows, n_z, n_x,
    sky_hbm, cov_hbm, cos_hbm, matrix,
    filtered_out, spectra_out,
    sky, cov, cos, cheb, cheb_x, part, parcel, landed, rest, landed_rest, mine, rows, cols,
    lhs, lhs_x, fj, total, share, line_landed, line_sum, plane_landed, result,
    load_sem, send1, recv1, send_rest, recv_rest, send2, recv2, send3, recv3,
    send4, recv4, send5, recv5, send6, recv6,
):
    r = lax.axis_index("prow")
    c = lax.axis_index("pcol")
    n = n_z * n_x
    z, x = c // n_x, lax.rem(c, n_x)
    q, h = c // 2, lax.rem(c, 2)
    half_n = n // 2
    maps = sky.shape[1]
    per, width = parcel.shape[1], parcel.shape[2]
    order = rank_order(n_z, n_x)
    diagonal = r == q
    off = r != q
    side = jnp.where(r > q, h, 1 - h)
    barrier = pltpu.get_barrier_semaphore()

    def peer(spot):
        return lax.rem(z + spot[0], n_z) * n_x + lax.rem(x + spot[1], n_x)

    def line(e):
        return lax.rem(r + e, n_rows)

    def signal(device):
        pl.semaphore_signal(barrier, inc=1, device_id=device, device_id_type=MESH)

    def copy(src, dst, send, recv, device):
        return pltpu.make_async_remote_copy(
            src_ref=src, dst_ref=dst, send_sem=send, recv_sem=recv,
            device_id=device, device_id_type=MESH,
        )

    first = [jnp.where(diagonal, 2 * h, 2 * side), jnp.where(diagonal, 1 + 2 * h, 2 * side)]
    second = [jnp.where(diagonal, 2 * h + 1, 2 * side + 1), jnp.where(diagonal, 2 - 2 * h, 2 * side + 1)]
    spare = 2 - h

    def tile_at(index):
        return pl.ds(pl.multiple_of(index * TILE, TILE), TILE)

    loads = [
        pltpu.make_async_copy(sky_hbm, sky, load_sem.at[0]),
        pltpu.make_async_copy(cov_hbm, cov, load_sem.at[1]),
    ]
    for t in range(2):
        for s, row in enumerate((first[t], second[t])):
            loads.append(
                pltpu.make_async_copy(
                    cos_hbm.at[tile_at(row), pl.ds(t * TILE, TILE)],
                    cos.at[pl.ds((2 * t + s) * TILE, TILE)],
                    load_sem.at[2 + 2 * t + s],
                )
            )
    spare_load = pltpu.make_async_copy(
        cos_hbm.at[tile_at(spare), tile_at(h)], cos.at[pl.ds(4 * TILE, TILE)], load_sem.at[6]
    )
    for load in loads:
        load.start()

    @pl.when(diagonal)
    def _():
        spare_load.start()

    for spot in order:
        signal((r, peer(spot)))
    for e in LINE:
        signal((line(e), c))

    @pl.when(off)
    def _():
        for j in range(half_n):
            signal((q, h * half_n + j))

    loads[0].wait()
    loads[1].wait()
    sky_t = sky[...].astype(jnp.float32).T.astype(jnp.bfloat16)
    wide = 2 * width
    for g in range(cov.shape[0] // wide):
        value = lax.dot_general(
            sky_t, cov[g * wide : (g + 1) * wide, :], (((1,), (1,)), ((), ())),
            preferred_element_type=jnp.float32,
        )
        for a in range(2):
            for b in range(maps // per):
                k = (2 * g + a) * (maps // per) + b
                piece = value[b * per : (b + 1) * per, a * width : (a + 1) * width]
                part[k] = piece
                parcel[k] = piece.astype(jnp.bfloat16)

    pl.semaphore_wait(barrier, len(order) + 2 * (n_rows - 1))

    def scatter(s):
        to = peer(order[s])
        return copy(parcel.at[to], landed.at[s], send1.at[s], recv1.at[s], (r, to))

    for s in range(len(order)):
        scatter(s).start()

    def scatter_rest(j):
        to = h * half_n + j
        return copy(rest.at[j], landed_rest, send_rest.at[j], recv_rest, (r, to))

    @pl.when(diagonal)
    def _():
        for j in range(half_n):
            k = h * half_n + j
            rest[j] = (part[k] - parcel[k].astype(jnp.float32)).astype(jnp.bfloat16)
        for j in range(half_n):
            @pl.when(c != h * half_n + j)
            def _():
                scatter_rest(j).start()

    def generate(base, store):
        def strip(s, carry):
            at = pl.multiple_of(s * STRIP, STRIP)
            value = cos[pl.ds(base + at, STRIP), :]
            double = value + value
            before, now = value, jnp.ones_like(value)
            for k in range(LEVELS):
                store(k, at, now.astype(jnp.bfloat16))
                before, now = now, double * now - before
            return carry

        return strip

    def generate_pair(t):
        def store(k, at, value):
            cheb[k, t, pl.ds(at, STRIP), :] = value

        loads[2 + 2 * t].wait()
        loads[3 + 2 * t].wait()
        lax.fori_loop(0, 2 * TILE // STRIP, generate(2 * t * TILE, store), 0)

    generate_pair(0)

    sum_value = part[c]
    for s in range(len(order)):
        scatter(s).wait_recv()
        sum_value = sum_value + landed[s].astype(jnp.float32)
    part[c] = sum_value
    has_rest = c != 2 * r + c // half_n

    @pl.when(has_rest)
    def _():
        copy(rest.at[0], landed_rest, send_rest.at[0], recv_rest, (r, 2 * r + c // half_n)).wait_recv()
        part[c] = part[c] + landed_rest[...].astype(jnp.float32)

    mine[...] = part[c].astype(jnp.bfloat16)
    chunk_half = c // half_n

    def place(ref, k):
        return ref.at[
            pl.ds(pl.multiple_of(lax.rem(k, 2) * per, per), per),
            pl.ds(pl.multiple_of((k // 2) * width, width), width),
        ]

    def gather(s):
        return copy(mine, place(rows, c), send2.at[s], recv2.at[c], (r, peer(order[s])))

    def gathered(k):
        return copy(mine, place(rows, k), send2.at[0], recv2.at[k], (r, k))

    def column(e):
        return copy(
            mine, place(cols, lax.rem(c, half_n)), send3.at[e - 1], recv3.at[lax.rem(c, half_n)],
            (line(e), 2 * r + chunk_half),
        )

    def wanted(to):
        parity = jnp.where(to // 2 < r, chunk_half, 1 - chunk_half)
        return jnp.logical_or(to // 2 == r, lax.rem(to, 2) == parity)

    for e in LINE[:4]:
        column(e).start()
    for s in range(len(order)):
        @pl.when(wanted(peer(order[s])))
        def _():
            gather(s).start()
    for e in LINE[4:]:
        column(e).start()
    rows[
        pl.ds(pl.multiple_of(lax.rem(c, 2) * per, per), per),
        pl.ds(pl.multiple_of((c // 2) * width, width), width),
    ] = mine[...]

    generate_pair(1)

    @pl.when(diagonal)
    def _():
        def store(k, at, value):
            cheb_x[k, pl.ds(at, STRIP), :] = value

        spare_load.wait()
        lax.fori_loop(0, TILE // STRIP, generate(4 * TILE, store), 0)

    for s in range(len(order)):
        @pl.when(jnp.logical_not(wanted(peer(order[s]))))
        def _():
            gather(s).start()

    for k in range(n):
        needed = jnp.logical_or(diagonal, side == k // half_n)

        @pl.when(jnp.logical_and(needed, c != k))
        def _():
            gathered(k).wait_recv()

    @pl.when(off)
    def _():
        for j in range(half_n):
            copy(
                mine, place(cols, j), send3.at[0], recv3.at[j], (q, h * half_n + j)
            ).wait_recv()

    @pl.when(diagonal)
    def _():
        size = cols.shape[1]
        cols[...] = rows[:, pl.ds(pl.multiple_of(h * size, size), size)]

    weight = jnp.where(diagonal, 1, 2).astype(jnp.float32)
    for t in range(2):
        lhs[t, :, :TILE] = (rows[:, tile_at(first[t])].astype(jnp.float32) * weight).astype(jnp.bfloat16)
        lhs[t, :, TILE:] = (rows[:, tile_at(second[t])].astype(jnp.float32) * 2.0).astype(jnp.bfloat16)
        fj[t] = cols[:, t * TILE : (t + 1) * TILE].astype(jnp.float32)

    @pl.when(diagonal)
    def _():
        lhs_x[...] = (rows[:, tile_at(spare)].astype(jnp.float32) * 2.0).astype(jnp.bfloat16)

    total[...] = jnp.zeros_like(total)

    def levels(with_spare):
        def body(step, carry):
            acc = total[...]
            for u in range(UNROLL):
                k = step * UNROLL + u
                prod = None
                for t in range(2):
                    image = jnp.dot(lhs[t], cheb[k, t], preferred_element_type=jnp.float32)
                    term = image * fj[t]
                    prod = term if prod is None else prod + term
                if with_spare:
                    image = jnp.dot(lhs_x[...], cheb_x[k], preferred_element_type=jnp.float32)
                    prod = prod + image * fj[h]
                narrow = prod[:, :LANES] + prod[:, LANES:]
                moment = jnp.sum(narrow, axis=-1, keepdims=True)
                acc = acc + moment * matrix[pl.ds(k, 1), :]
            total[...] = acc
            return carry

        lax.fori_loop(0, LEVELS // UNROLL, body, 0)

    @pl.when(off)
    def _():
        levels(False)

    @pl.when(diagonal)
    def _():
        levels(True)

    share[...] = total[...].T[:L]

    piece = L // n_rows

    def block(k):
        return pl.ds(pl.multiple_of(k * piece, piece), piece)

    def reduce_line(e):
        return copy(
            share.at[block(line(e))], line_landed.at[e - 1], send4.at[e - 1], recv4.at[e - 1], (line(e), c)
        )

    def exchange(s):
        return copy(line_sum, plane_landed.at[c], send5.at[s], recv5.at[s], (r, peer(order[s])))

    def spread_line(e, k):
        return copy(result, spectra_out.at[block(k)], send6.at[e - 1], recv6.at[e - 1], (line(e), c))

    for e in LINE:
        reduce_line(e).start()

    for k in range(n):
        needed = jnp.logical_or(diagonal, side == k // half_n)

        @pl.when(jnp.logical_and(jnp.logical_not(needed), c != k))
        def _():
            gathered(k).wait_recv()

    def turn(g, carry):
        at = pl.ds(pl.multiple_of(g * LANES, LANES), LANES)
        filtered_out[at, :] = rows[:, at].astype(jnp.float32).T.astype(jnp.bfloat16)
        return carry

    lax.fori_loop(0, rows.shape[1] // LANES, turn, 0)

    for e in LINE:
        reduce_line(e).wait_recv()
    value = share[block(r)]
    for e in range(1, n_rows):
        value = value + line_landed[e - 1]
    line_sum[...] = value
    for s in range(len(order)):
        exchange(s).start()
    plane_landed[c] = value
    for s in range(len(order)):
        exchange(s).wait_recv()
    value = plane_landed[0]
    for k in range(1, n):
        value = value + plane_landed[k]
    result[...] = value
    for e in LINE:
        spread_line(e, r).start()
    spectra_out[block(r)] = value
    for e in LINE:
        spread_line(e, lax.rem(r - e + n_rows, n_rows)).wait_recv()

    for s in range(len(order)):
        scatter(s).wait_send()
        gather(s).wait_send()
        exchange(s).wait_send()
    for e in LINE:
        column(e).wait_send()
        reduce_line(e).wait_send()
        spread_line(e, r).wait_send()

    @pl.when(diagonal)
    def _():
        for j in range(half_n):
            @pl.when(c != h * half_n + j)
            def _():
                scatter_rest(j).wait_send()


def per_device(npix, n_rows, n_cols, inverse_cov, cosines, sky_maps):
    n_z = n_cols // N_X
    n = n_cols
    size, cols_here = inverse_cov.shape
    maps = sky_maps.shape[1]
    per, width = maps // 2, 2 * size // n
    piece = L // n_rows
    vmem = pl.BlockSpec(memory_space=pltpu.VMEM)
    anywhere = pl.BlockSpec(memory_space=pl.ANY)
    bf16, f32 = jnp.bfloat16, jnp.float32
    plane = pltpu.SemaphoreType.DMA((n - 1,))
    line = pltpu.SemaphoreType.DMA((n_rows - 1,))
    half = pltpu.SemaphoreType.DMA((n // 2,))
    filtered, spectra = pl.pallas_call(
        functools.partial(qml_kernel, n_rows, n_z, N_X),
        out_shape=(
            jax.ShapeDtypeStruct((size, maps), bf16),
            jax.ShapeDtypeStruct((L, maps), f32),
        ),
        in_specs=[anywhere, anywhere, anywhere, vmem],
        out_specs=(vmem, vmem),
        scratch_shapes=[
            pltpu.VMEM(sky_maps.shape, bf16),
            pltpu.VMEM(inverse_cov.shape, bf16),
            pltpu.VMEM((5 * TILE, TILE), f32),
            pltpu.VMEM((LEVELS, 2, 2 * TILE, TILE), bf16),
            pltpu.VMEM((LEVELS, TILE, TILE), bf16),
            pltpu.VMEM((n, per, width), f32),
            pltpu.VMEM((n, per, width), bf16),
            pltpu.VMEM((n - 1, per, width), bf16),
            pltpu.VMEM((n // 2, per, width), bf16),
            pltpu.VMEM((per, width), bf16),
            pltpu.VMEM((per, width), bf16),
            pltpu.VMEM((maps, size), bf16),
            pltpu.VMEM((maps, cols_here), bf16),
            pltpu.VMEM((2, maps, 2 * TILE), bf16),
            pltpu.VMEM((maps, TILE), bf16),
            pltpu.VMEM((2, maps, TILE), f32),
            pltpu.VMEM((maps, LANES), f32),
            pltpu.VMEM((L, maps), f32),
            pltpu.VMEM((n_rows - 1, piece, maps), f32),
            pltpu.VMEM((piece, maps), f32),
            pltpu.VMEM((n, piece, maps), f32),
            pltpu.VMEM((piece, maps), f32),
            pltpu.SemaphoreType.DMA((7,)),
            plane, plane, half, pltpu.SemaphoreType.DMA, plane, pltpu.SemaphoreType.DMA((n,)),
            line, half, line, line, plane, plane, line, line,
        ],
        compiler_params=pltpu.CompilerParams(
            collective_id=1, has_side_effects=True, vmem_limit_bytes=60 * 2**20
        ),
        name="qml",
    )(sky_maps, inverse_cov, cosines, jnp.asarray(transform_matrix(npix)))
    return filtered, spectra


def solution(mesh):
    in_specs = (P("prow", "pcol"), P("prow", "pcol"), P("pcol", None))
    out_specs = (P("prow", None), P())
    n_rows, n_cols = mesh.shape["prow"], mesh.shape["pcol"]

    def whole(inverse_cov, cosines, sky_maps):
        npix = cosines.shape[0]
        step = jax.shard_map(
            functools.partial(per_device, npix, n_rows, n_cols),
            mesh=mesh, in_specs=in_specs, out_specs=out_specs, check_vma=False,
        )
        return step(inverse_cov, cosines, sky_maps)

    return whole
```

```python
import functools
import math

import jax
import jax.numpy as jnp
import numpy as np
from jax import lax
from jax.experimental import pallas as pl
from jax.experimental.pallas import tpu as pltpu
from jax.sharding import PartitionSpec as P

L = 64
LMIN = 2
TOP = LMIN + L - 1
LEVELS = TOP + 1
UNROLL = 6
TILE = 256
STRIP = 32
N_X = 4
LANES = 128
MESH = pl.DeviceIdType.MESH


def transform_matrix(npix):
    a = [math.comb(2 * k, k) / 4.0**k for k in range(TOP + 1)]
    out = np.zeros((-(-LEVELS // 8) * 8, LANES))
    for l in range(LMIN, TOP + 1):
        for k in range(l + 1):
            out[abs(l - 2 * k), l - LMIN] += a[k] * a[l - k] * (2 * l + 1) / npix
    return out.astype(np.float32)


def rank_order(rows, cols):
    spots = [(dz, dx) for dz in range(rows) for dx in range(cols) if dz or dx]
    reach = lambda d, n: min(d, n - d)
    return sorted(spots, key=lambda s: -(reach(s[0], rows) + reach(s[1], cols)))


LINE = [4, 5, 3, 2, 6, 1, 7]


def qml_kernel(
    n_rows, n_z, n_x,
    sky_hbm, cov_hbm, cos_hbm, matrix_hbm,
    rows, spectra_out,
    sky, cov, cos, matrix, cheb, cheb_x, part, parcel, landed, rest, landed_rest, mine, cols,
    lhs, lhs_x, fj, total, share, line_landed, line_sum, plane_landed, result,
    load_sem, send1, recv1, send_rest, recv_rest, send2, recv2, send3, recv3,
    send4, recv4, send5, recv5, send6, recv6,
):
    r = lax.axis_index("prow")
    c = lax.axis_index("pcol")
    n = n_z * n_x
    z, x = c // n_x, lax.rem(c, n_x)
    q, h = c // 2, lax.rem(c, 2)
    half_n = n // 2
    maps = sky.shape[0]
    per, width = parcel.shape[1], parcel.shape[2]
    order = rank_order(n_z, n_x)
    diagonal = r == q
    off = r != q
    side = jnp.where(r > q, h, 1 - h)
    barrier = pltpu.get_barrier_semaphore()

    def peer(spot):
        return lax.rem(z + spot[0], n_z) * n_x + lax.rem(x + spot[1], n_x)

    def line(e):
        return lax.rem(r + e, n_rows)

    def signal(device):
        pl.semaphore_signal(barrier, inc=1, device_id=device, device_id_type=MESH)

    def copy(src, dst, send, recv, device):
        return pltpu.make_async_remote_copy(
            src_ref=src, dst_ref=dst, send_sem=send, recv_sem=recv,
            device_id=device, device_id_type=MESH,
        )

    first = [jnp.where(diagonal, 2 * h, 2 * side), jnp.where(diagonal, 1 + 2 * h, 2 * side)]
    second = [jnp.where(diagonal, 2 * h + 1, 2 * side + 1), jnp.where(diagonal, 2 - 2 * h, 2 * side + 1)]
    spare = 2 - h

    def tile_at(index):
        return pl.ds(pl.multiple_of(index * TILE, TILE), TILE)

    loads = [
        pltpu.make_async_copy(sky_hbm, sky, load_sem.at[0]),
        pltpu.make_async_copy(cov_hbm, cov, load_sem.at[1]),
    ]
    for t in range(2):
        for s, row in enumerate((first[t], second[t])):
            loads.append(
                pltpu.make_async_copy(
                    cos_hbm.at[tile_at(row), pl.ds(t * TILE, TILE)],
                    cos.at[pl.ds((2 * t + s) * TILE, TILE)],
                    load_sem.at[2 + 2 * t + s],
                )
            )
    matrix_load = pltpu.make_async_copy(matrix_hbm, matrix, load_sem.at[7])
    spare_load = pltpu.make_async_copy(
        cos_hbm.at[tile_at(spare), tile_at(h)], cos.at[pl.ds(4 * TILE, TILE)], load_sem.at[6]
    )
    for load in loads:
        load.start()
    matrix_load.start()

    @pl.when(diagonal)
    def _():
        spare_load.start()

    for spot in order:
        signal((r, peer(spot)))
    for e in LINE:
        signal((line(e), c))

    @pl.when(off)
    def _():
        for j in range(half_n):
            signal((q, h * half_n + j))

    loads[0].wait()
    loads[1].wait()
    wide = 2 * width
    for g in range(cov.shape[0] // wide):
        value = lax.dot_general(
            sky[...], cov[g * wide : (g + 1) * wide, :], (((1,), (1,)), ((), ())),
            preferred_element_type=jnp.float32,
        )
        for a in range(2):
            for b in range(maps // per):
                k = (2 * g + a) * (maps // per) + b
                piece = value[b * per : (b + 1) * per, a * width : (a + 1) * width]
                part[k] = piece
                parcel[k] = piece.astype(jnp.bfloat16)

    pl.semaphore_wait(barrier, len(order) + 2 * (n_rows - 1))

    def scatter(s):
        to = peer(order[s])
        return copy(parcel.at[to], landed.at[s], send1.at[s], recv1.at[s], (r, to))

    for s in range(len(order)):
        scatter(s).start()

    def scatter_rest(j):
        to = h * half_n + j
        return copy(rest.at[j], landed_rest, send_rest.at[j], recv_rest, (r, to))

    @pl.when(diagonal)
    def _():
        for j in range(half_n):
            k = h * half_n + j
            rest[j] = (part[k] - parcel[k].astype(jnp.float32)).astype(jnp.bfloat16)
        for j in range(half_n):
            @pl.when(c != h * half_n + j)
            def _():
                scatter_rest(j).start()

    def generate(base, store):
        def strip(s, carry):
            at = pl.multiple_of(s * STRIP, STRIP)
            value = cos[pl.ds(base + at, STRIP), :]
            double = value + value
            before, now = value, jnp.ones_like(value)
            for k in range(LEVELS):
                store(k, at, now.astype(jnp.bfloat16))
                before, now = now, double * now - before
            return carry

        return strip

    def generate_pair(t):
        def store(k, at, value):
            cheb[k, t, pl.ds(at, STRIP), :] = value

        loads[2 + 2 * t].wait()
        loads[3 + 2 * t].wait()
        lax.fori_loop(0, 2 * TILE // STRIP, generate(2 * t * TILE, store), 0)

    generate_pair(0)

    sum_value = part[c]
    for s in range(len(order)):
        scatter(s).wait_recv()
        sum_value = sum_value + landed[s].astype(jnp.float32)
    part[c] = sum_value
    has_rest = c != 2 * r + c // half_n

    @pl.when(has_rest)
    def _():
        copy(rest.at[0], landed_rest, send_rest.at[0], recv_rest, (r, 2 * r + c // half_n)).wait_recv()
        part[c] = part[c] + landed_rest[...].astype(jnp.float32)

    mine[...] = part[c].astype(jnp.bfloat16)
    chunk_half = c // half_n

    def place(ref, k):
        return ref.at[
            pl.ds(pl.multiple_of(lax.rem(k, 2) * per, per), per),
            pl.ds(pl.multiple_of((k // 2) * width, width), width),
        ]

    def gather(s):
        return copy(mine, place(rows, c), send2.at[s], recv2.at[c], (r, peer(order[s])))

    def gathered(k):
        return copy(mine, place(rows, k), send2.at[0], recv2.at[k], (r, k))

    def column(e):
        return copy(
            mine, place(cols, lax.rem(c, half_n)), send3.at[e - 1], recv3.at[lax.rem(c, half_n)],
            (line(e), 2 * r + chunk_half),
        )

    def wanted(to):
        parity = jnp.where(to // 2 < r, chunk_half, 1 - chunk_half)
        return jnp.logical_or(to // 2 == r, lax.rem(to, 2) == parity)

    for e in LINE[:4]:
        column(e).start()
    for s in range(len(order)):
        @pl.when(wanted(peer(order[s])))
        def _():
            gather(s).start()
    for e in LINE[4:]:
        column(e).start()
    rows[
        pl.ds(pl.multiple_of(lax.rem(c, 2) * per, per), per),
        pl.ds(pl.multiple_of((c // 2) * width, width), width),
    ] = mine[...]

    generate_pair(1)

    @pl.when(diagonal)
    def _():
        def store(k, at, value):
            cheb_x[k, pl.ds(at, STRIP), :] = value

        spare_load.wait()
        lax.fori_loop(0, TILE // STRIP, generate(4 * TILE, store), 0)

    for s in range(len(order)):
        @pl.when(jnp.logical_not(wanted(peer(order[s]))))
        def _():
            gather(s).start()

    for k in range(n):
        needed = jnp.logical_or(diagonal, side == k // half_n)

        @pl.when(jnp.logical_and(needed, c != k))
        def _():
            gathered(k).wait_recv()

    @pl.when(off)
    def _():
        for j in range(half_n):
            copy(
                mine, place(cols, j), send3.at[0], recv3.at[j], (q, h * half_n + j)
            ).wait_recv()

    @pl.when(diagonal)
    def _():
        size = cols.shape[1]
        cols[...] = rows[:, pl.ds(pl.multiple_of(h * size, size), size)]

    weight = jnp.where(diagonal, 1, 2).astype(jnp.float32)
    for t in range(2):
        lhs[t, :, :TILE] = (rows[:, tile_at(first[t])].astype(jnp.float32) * weight).astype(jnp.bfloat16)
        lhs[t, :, TILE:] = (rows[:, tile_at(second[t])].astype(jnp.float32) * 2.0).astype(jnp.bfloat16)
        fj[t] = cols[:, t * TILE : (t + 1) * TILE].astype(jnp.float32)

    @pl.when(diagonal)
    def _():
        lhs_x[...] = (rows[:, tile_at(spare)].astype(jnp.float32) * 2.0).astype(jnp.bfloat16)

    matrix_load.wait()
    total[...] = jnp.zeros_like(total)

    def levels(with_spare):
        def body(step, carry):
            acc = total[...]
            for u in range(UNROLL):
                k = step * UNROLL + u
                prod = None
                for t in range(2):
                    image = jnp.dot(lhs[t], cheb[k, t], preferred_element_type=jnp.float32)
                    term = image * fj[t]
                    prod = term if prod is None else prod + term
                if with_spare:
                    image = jnp.dot(lhs_x[...], cheb_x[k], preferred_element_type=jnp.float32)
                    prod = prod + image * fj[h]
                narrow = prod[:, :LANES] + prod[:, LANES:]
                moment = jnp.sum(narrow, axis=-1, keepdims=True)
                acc = acc + moment * matrix[pl.ds(k, 1), :]
            total[...] = acc
            return carry

        lax.fori_loop(0, LEVELS // UNROLL, body, 0)

    @pl.when(off)
    def _():
        levels(False)

    @pl.when(diagonal)
    def _():
        levels(True)

    share[...] = total[...].T[:L]

    piece = L // n_rows

    def block(k):
        return pl.ds(pl.multiple_of(k * piece, piece), piece)

    def reduce_line(e):
        return copy(
            share.at[block(line(e))], line_landed.at[e - 1], send4.at[e - 1], recv4.at[e - 1], (line(e), c)
        )

    def exchange(s):
        return copy(line_sum, plane_landed.at[c], send5.at[s], recv5.at[s], (r, peer(order[s])))

    def spread_line(e, k):
        return copy(result, spectra_out.at[block(k)], send6.at[e - 1], recv6.at[e - 1], (line(e), c))

    for e in LINE:
        reduce_line(e).start()

    for k in range(n):
        needed = jnp.logical_or(diagonal, side == k // half_n)

        @pl.when(jnp.logical_and(jnp.logical_not(needed), c != k))
        def _():
            gathered(k).wait_recv()

    for e in LINE:
        reduce_line(e).wait_recv()
    value = share[block(r)]
    for e in range(1, n_rows):
        value = value + line_landed[e - 1]
    line_sum[...] = value
    for s in range(len(order)):
        exchange(s).start()
    plane_landed[c] = value
    for s in range(len(order)):
        exchange(s).wait_recv()
    value = plane_landed[0]
    for k in range(1, n):
        value = value + plane_landed[k]
    result[...] = value
    for e in LINE:
        spread_line(e, r).start()
    spectra_out[block(r)] = value
    for e in LINE:
        spread_line(e, lax.rem(r - e + n_rows, n_rows)).wait_recv()

    for s in range(len(order)):
        scatter(s).wait_send()
        gather(s).wait_send()
        exchange(s).wait_send()
    for e in LINE:
        column(e).wait_send()
        reduce_line(e).wait_send()
        spread_line(e, r).wait_send()

    @pl.when(diagonal)
    def _():
        for j in range(half_n):
            @pl.when(c != h * half_n + j)
            def _():
                scatter_rest(j).wait_send()


def per_device(npix, n_rows, n_cols, inverse_cov, cosines, sky_maps):
    n_z = n_cols // N_X
    n = n_cols
    size, cols_here = inverse_cov.shape
    maps = sky_maps.shape[1]
    sky_t = sky_maps.T
    per, width = maps // 2, 2 * size // n
    piece = L // n_rows
    vmem = pl.BlockSpec(memory_space=pltpu.VMEM)
    hbm = pl.BlockSpec(memory_space=pltpu.HBM)
    matrix = jnp.asarray(transform_matrix(npix))
    inputs = (sky_t, inverse_cov, cosines, matrix)
    bf16, f32 = jnp.bfloat16, jnp.float32
    plane = pltpu.SemaphoreType.DMA((n - 1,))
    line = pltpu.SemaphoreType.DMA((n_rows - 1,))
    half = pltpu.SemaphoreType.DMA((n // 2,))
    filtered, spectra = pl.pallas_call(
        functools.partial(qml_kernel, n_rows, n_z, N_X),
        out_shape=(
            jax.ShapeDtypeStruct((maps, size), bf16),
            jax.ShapeDtypeStruct((L, maps), f32),
        ),
        in_specs=[hbm] * len(inputs),
        out_specs=(vmem, vmem),
        scratch_shapes=[
            pltpu.VMEM(sky_t.shape, bf16),
            pltpu.VMEM(inverse_cov.shape, bf16),
            pltpu.VMEM((5 * TILE, TILE), f32),
            pltpu.VMEM(matrix.shape, f32),
            pltpu.VMEM((LEVELS, 2, 2 * TILE, TILE), bf16),
            pltpu.VMEM((LEVELS, TILE, TILE), bf16),
            pltpu.VMEM((n, per, width), f32),
            pltpu.VMEM((n, per, width), bf16),
            pltpu.VMEM((n - 1, per, width), bf16),
            pltpu.VMEM((n // 2, per, width), bf16),
            pltpu.VMEM((per, width), bf16),
            pltpu.VMEM((per, width), bf16),
            pltpu.VMEM((maps, cols_here), bf16),
            pltpu.VMEM((2, maps, 2 * TILE), bf16),
            pltpu.VMEM((maps, TILE), bf16),
            pltpu.VMEM((2, maps, TILE), f32),
            pltpu.VMEM((maps, LANES), f32),
            pltpu.VMEM((L, maps), f32),
            pltpu.VMEM((n_rows - 1, piece, maps), f32),
            pltpu.VMEM((piece, maps), f32),
            pltpu.VMEM((n, piece, maps), f32),
            pltpu.VMEM((piece, maps), f32),
            pltpu.SemaphoreType.DMA((8,)),
            plane, plane, half, pltpu.SemaphoreType.DMA, plane, pltpu.SemaphoreType.DMA((n,)),
            line, half, line, line, plane, plane, line, line,
        ],
        compiler_params=pltpu.CompilerParams(
            collective_id=1, has_side_effects=True, vmem_limit_bytes=50 * 2**20
        ),
        name="qml",
    )(*[pltpu.with_memory_space_constraint(value, pltpu.HBM) for value in inputs])
    return filtered.T, spectra


def solution(mesh):
    in_specs = (P("prow", "pcol"), P("prow", "pcol"), P("pcol", None))
    out_specs = (P("prow", None), P())
    n_rows, n_cols = mesh.shape["prow"], mesh.shape["pcol"]

    def whole(inverse_cov, cosines, sky_maps):
        npix = cosines.shape[0]
        step = jax.shard_map(
            functools.partial(per_device, npix, n_rows, n_cols),
            mesh=mesh, in_specs=in_specs, out_specs=out_specs, check_vma=False,
        )
        return step(inverse_cov, cosines, sky_maps)

    return whole
```

```python
import functools
import math

import jax
import jax.numpy as jnp
import numpy as np
from jax import lax
from jax.experimental import pallas as pl
from jax.experimental.pallas import tpu as pltpu
from jax.sharding import PartitionSpec as P

L = 64
LMIN = 2
TOP = LMIN + L - 1
LEVELS = TOP + 1
UNROLL = 22
TILE = 256
STRIP = 32
N_X = 4
LANES = 128
MESH = pl.DeviceIdType.MESH


def transform_matrix(npix):
    a = [math.comb(2 * k, k) / 4.0**k for k in range(TOP + 1)]
    out = np.zeros((-(-LEVELS // 8) * 8, LANES))
    for l in range(LMIN, TOP + 1):
        for k in range(l + 1):
            out[abs(l - 2 * k), l - LMIN] += a[k] * a[l - k] * (2 * l + 1) / npix
    return out.astype(np.float32)


def rank_order(rows, cols):
    spots = [(dz, dx) for dz in range(rows) for dx in range(cols) if dz or dx]
    reach = lambda d, n: min(d, n - d)
    return sorted(spots, key=lambda s: -(reach(s[0], rows) + reach(s[1], cols)))


LINE = [4, 5, 3, 2, 6, 1, 7]


def qml_kernel(
    n_rows, n_z, n_x,
    sky_hbm, cov_hbm, cos_hbm, matrix_hbm,
    rows, spectra_out,
    sky, cov, cos, matrix, cheb, cheb_x, part, parcel, landed, rest, landed_rest, mine, cols,
    lhs, lhs_x, fj, total, share, line_landed, line_sum, plane_landed, result,
    load_sem, send1, recv1, send_rest, recv_rest, send2, recv2, send3, recv3,
    send4, recv4, send5, recv5, send6, recv6,
):
    r = lax.axis_index("prow")
    c = lax.axis_index("pcol")
    n = n_z * n_x
    z, x = c // n_x, lax.rem(c, n_x)
    q, h = c // 2, lax.rem(c, 2)
    half_n = n // 2
    maps = sky.shape[0]
    per, width = parcel.shape[1], parcel.shape[2]
    order = rank_order(n_z, n_x)
    diagonal = r == q
    off = r != q
    side = jnp.where(r > q, h, 1 - h)
    barrier = pltpu.get_barrier_semaphore()

    def peer(spot):
        return lax.rem(z + spot[0], n_z) * n_x + lax.rem(x + spot[1], n_x)

    def line(e):
        return lax.rem(r + e, n_rows)

    def turn(row):
        return n_x // 2 * lax.rem(row, 2) + n_x - 1

    def chunk_of(row, col):
        return lax.rem(lax.rem(col, n_x) - turn(row) + 2 * n_x, n_x) * n_z + col // n_x

    def owner(row, k):
        return (k % n_z if isinstance(k, int) else lax.rem(k, n_z)) * n_x + lax.rem(k // n_z + turn(row), n_x)

    me = chunk_of(r, c)

    def signal(device):
        pl.semaphore_signal(barrier, inc=1, device_id=device, device_id_type=MESH)

    def copy(src, dst, send, recv, device):
        return pltpu.make_async_remote_copy(
            src_ref=src, dst_ref=dst, send_sem=send, recv_sem=recv,
            device_id=device, device_id_type=MESH,
        )

    first = [jnp.where(diagonal, 2 * h, 2 * side), jnp.where(diagonal, 1 + 2 * h, 2 * side)]
    second = [jnp.where(diagonal, 2 * h + 1, 2 * side + 1), jnp.where(diagonal, 2 - 2 * h, 2 * side + 1)]
    spare = 2 - h

    def tile_at(index):
        return pl.ds(pl.multiple_of(index * TILE, TILE), TILE)

    loads = [
        pltpu.make_async_copy(sky_hbm, sky, load_sem.at[0]),
        pltpu.make_async_copy(cov_hbm, cov, load_sem.at[1]),
    ]
    for t in range(2):
        for s, row in enumerate((first[t], second[t])):
            loads.append(
                pltpu.make_async_copy(
                    cos_hbm.at[tile_at(row), pl.ds(t * TILE, TILE)],
                    cos.at[pl.ds((2 * t + s) * TILE, TILE)],
                    load_sem.at[2 + 2 * t + s],
                )
            )
    matrix_load = pltpu.make_async_copy(matrix_hbm, matrix, load_sem.at[7])
    spare_load = pltpu.make_async_copy(
        cos_hbm.at[tile_at(spare), tile_at(h)], cos.at[pl.ds(4 * TILE, TILE)], load_sem.at[6]
    )
    for load in loads:
        load.start()
    matrix_load.start()

    @pl.when(diagonal)
    def _():
        spare_load.start()

    for spot in order:
        signal((r, peer(spot)))
    for e in LINE:
        signal((line(e), c))

    @pl.when(off)
    def _():
        for j in range(half_n):
            signal((q, owner(q, h * half_n + j)))

    loads[0].wait()
    loads[1].wait()
    wide = 2 * width
    for g in range(cov.shape[0] // wide):
        value = lax.dot_general(
            sky[...], cov[g * wide : (g + 1) * wide, :], (((1,), (1,)), ((), ())),
            preferred_element_type=jnp.float32,
        )
        for a in range(2):
            for b in range(maps // per):
                k = (2 * g + a) * (maps // per) + b
                piece = value[b * per : (b + 1) * per, a * width : (a + 1) * width]
                part[k] = piece
                parcel[k] = piece.astype(jnp.bfloat16)

    pl.semaphore_wait(barrier, len(order) + 2 * (n_rows - 1))

    def scatter(s):
        to = peer(order[s])
        return copy(parcel.at[chunk_of(r, to)], landed.at[s], send1.at[s], recv1.at[s], (r, to))

    for s in range(len(order)):
        scatter(s).start()

    def scatter_rest(j):
        to = owner(r, h * half_n + j)
        return copy(rest.at[j], landed_rest, send_rest.at[j], recv_rest, (r, to))

    @pl.when(diagonal)
    def _():
        for j in range(half_n):
            k = h * half_n + j
            rest[j] = (part[k] - parcel[k].astype(jnp.float32)).astype(jnp.bfloat16)
        for j in range(half_n):
            @pl.when(me != h * half_n + j)
            def _():
                scatter_rest(j).start()

    def generate(base, store):
        def strip(s, carry):
            at = pl.multiple_of(s * STRIP, STRIP)
            value = cos[pl.ds(base + at, STRIP), :]
            double = value + value
            before, now = value, jnp.ones_like(value)
            for k in range(LEVELS):
                store(k, at, now.astype(jnp.bfloat16))
                before, now = now, double * now - before
            return carry

        return strip

    def generate_pair(t):
        def store(k, at, value):
            cheb[k, t, pl.ds(at, STRIP), :] = value

        loads[2 + 2 * t].wait()
        loads[3 + 2 * t].wait()
        lax.fori_loop(0, 2 * TILE // STRIP, generate(2 * t * TILE, store), 0)

    generate_pair(0)

    sum_value = part[me]
    for s in range(len(order)):
        scatter(s).wait_recv()
        sum_value = sum_value + landed[s].astype(jnp.float32)
    part[me] = sum_value
    chunk_half = me // half_n
    has_rest = c != 2 * r + chunk_half

    @pl.when(has_rest)
    def _():
        copy(rest.at[0], landed_rest, send_rest.at[0], recv_rest, (r, 2 * r + chunk_half)).wait_recv()
        part[me] = part[me] + landed_rest[...].astype(jnp.float32)

    mine[...] = part[me].astype(jnp.bfloat16)

    def place(ref, k):
        return ref.at[
            pl.ds(pl.multiple_of(lax.rem(k, 2) * per, per), per),
            pl.ds(pl.multiple_of((k // 2) * width, width), width),
        ]

    def gather(s):
        return copy(mine, place(rows, me), send2.at[s], recv2.at[me], (r, peer(order[s])))

    def gathered(k):
        return copy(mine, place(rows, k), send2.at[0], recv2.at[k], (r, owner(r, k)))

    def column(e):
        return copy(
            mine, place(cols, lax.rem(me, half_n)), send3.at[e - 1], recv3.at[lax.rem(me, half_n)],
            (line(e), 2 * r + chunk_half),
        )

    def wanted(to):
        parity = jnp.where(to // 2 < r, chunk_half, 1 - chunk_half)
        return jnp.logical_or(to // 2 == r, lax.rem(to, 2) == parity)

    for e in LINE[:4]:
        column(e).start()
    for s in range(len(order)):
        @pl.when(wanted(peer(order[s])))
        def _():
            gather(s).start()
    for e in LINE[4:]:
        column(e).start()
    rows[
        pl.ds(pl.multiple_of(lax.rem(me, 2) * per, per), per),
        pl.ds(pl.multiple_of((me // 2) * width, width), width),
    ] = mine[...]

    generate_pair(1)

    @pl.when(diagonal)
    def _():
        def store(k, at, value):
            cheb_x[k, pl.ds(at, STRIP), :] = value

        spare_load.wait()
        lax.fori_loop(0, TILE // STRIP, generate(4 * TILE, store), 0)

    for s in range(len(order)):
        @pl.when(jnp.logical_not(wanted(peer(order[s]))))
        def _():
            gather(s).start()

    for k in range(n):
        needed = jnp.logical_or(diagonal, side == k // half_n)

        @pl.when(jnp.logical_and(needed, me != k))
        def _():
            gathered(k).wait_recv()

    @pl.when(off)
    def _():
        for j in range(half_n):
            copy(
                mine, place(cols, j), send3.at[0], recv3.at[j], (q, owner(q, h * half_n + j))
            ).wait_recv()

    @pl.when(diagonal)
    def _():
        size = cols.shape[1]
        cols[...] = rows[:, pl.ds(pl.multiple_of(h * size, size), size)]

    weight = jnp.where(diagonal, 1, 2).astype(jnp.float32)
    for t in range(2):
        lhs[t, :, :TILE] = (rows[:, tile_at(first[t])].astype(jnp.float32) * weight).astype(jnp.bfloat16)
        lhs[t, :, TILE:] = (rows[:, tile_at(second[t])].astype(jnp.float32) * 2.0).astype(jnp.bfloat16)
        fj[t] = cols[:, t * TILE : (t + 1) * TILE].astype(jnp.float32)

    @pl.when(diagonal)
    def _():
        lhs_x[...] = (rows[:, tile_at(spare)].astype(jnp.float32) * 2.0).astype(jnp.bfloat16)

    matrix_load.wait()
    total[...] = jnp.zeros_like(total)

    def levels(with_spare):
        def body(step, carry):
            acc = total[...]
            for u in range(UNROLL):
                k = step * UNROLL + u
                prod = None
                for t in range(2):
                    image = jnp.dot(lhs[t], cheb[k, t], preferred_element_type=jnp.float32)
                    term = image * fj[t]
                    prod = term if prod is None else prod + term
                if with_spare:
                    image = jnp.dot(lhs_x[...], cheb_x[k], preferred_element_type=jnp.float32)
                    prod = prod + image * fj[h]
                narrow = prod[:, :LANES] + prod[:, LANES:]
                moment = jnp.sum(narrow, axis=-1, keepdims=True)
                acc = acc + moment * matrix[pl.ds(k, 1), :]
            total[...] = acc
            return carry

        lax.fori_loop(0, LEVELS // UNROLL, body, 0)

    @pl.when(off)
    def _():
        levels(False)

    @pl.when(diagonal)
    def _():
        levels(True)

    share[...] = total[...].T[:L]

    piece = L // n_rows

    def block(k):
        return pl.ds(pl.multiple_of(k * piece, piece), piece)

    def reduce_line(e):
        return copy(
            share.at[block(line(e))], line_landed.at[e - 1], send4.at[e - 1], recv4.at[e - 1], (line(e), c)
        )

    def exchange(s):
        return copy(line_sum, plane_landed.at[c], send5.at[s], recv5.at[s], (r, peer(order[s])))

    def spread_line(e, k):
        return copy(result, spectra_out.at[block(k)], send6.at[e - 1], recv6.at[e - 1], (line(e), c))

    for e in LINE:
        reduce_line(e).start()

    for k in range(n):
        needed = jnp.logical_or(diagonal, side == k // half_n)

        @pl.when(jnp.logical_and(jnp.logical_not(needed), me != k))
        def _():
            gathered(k).wait_recv()

    for e in LINE:
        reduce_line(e).wait_recv()
    value = share[block(r)]
    for e in range(1, n_rows):
        value = value + line_landed[e - 1]
    line_sum[...] = value
    for s in range(len(order)):
        exchange(s).start()
    plane_landed[c] = value
    for s in range(len(order)):
        exchange(s).wait_recv()
    value = plane_landed[0]
    for k in range(1, n):
        value = value + plane_landed[k]
    result[...] = value
    for e in LINE:
        spread_line(e, r).start()
    spectra_out[block(r)] = value
    for e in LINE:
        spread_line(e, lax.rem(r - e + n_rows, n_rows)).wait_recv()

    for s in range(len(order)):
        scatter(s).wait_send()
        gather(s).wait_send()
        exchange(s).wait_send()
    for e in LINE:
        column(e).wait_send()
        reduce_line(e).wait_send()
        spread_line(e, r).wait_send()

    @pl.when(diagonal)
    def _():
        for j in range(half_n):
            @pl.when(me != h * half_n + j)
            def _():
                scatter_rest(j).wait_send()


def per_device(npix, n_rows, n_cols, inverse_cov, cosines, sky_maps):
    n_z = n_cols // N_X
    n = n_cols
    size, cols_here = inverse_cov.shape
    maps = sky_maps.shape[1]
    sky_t = sky_maps.T
    per, width = maps // 2, 2 * size // n
    piece = L // n_rows
    vmem = pl.BlockSpec(memory_space=pltpu.VMEM)
    hbm = pl.BlockSpec(memory_space=pltpu.HBM)
    matrix = jnp.asarray(transform_matrix(npix))
    inputs = (sky_t, inverse_cov, cosines, matrix)
    bf16, f32 = jnp.bfloat16, jnp.float32
    plane = pltpu.SemaphoreType.DMA((n - 1,))
    line = pltpu.SemaphoreType.DMA((n_rows - 1,))
    half = pltpu.SemaphoreType.DMA((n // 2,))
    filtered, spectra = pl.pallas_call(
        functools.partial(qml_kernel, n_rows, n_z, N_X),
        out_shape=(
            jax.ShapeDtypeStruct((maps, size), bf16),
            jax.ShapeDtypeStruct((L, maps), f32),
        ),
        in_specs=[hbm] * len(inputs),
        out_specs=(vmem, vmem),
        scratch_shapes=[
            pltpu.VMEM(sky_t.shape, bf16),
            pltpu.VMEM(inverse_cov.shape, bf16),
            pltpu.VMEM((5 * TILE, TILE), f32),
            pltpu.VMEM(matrix.shape, f32),
            pltpu.VMEM((LEVELS, 2, 2 * TILE, TILE), bf16),
            pltpu.VMEM((LEVELS, TILE, TILE), bf16),
            pltpu.VMEM((n, per, width), f32),
            pltpu.VMEM((n, per, width), bf16),
            pltpu.VMEM((n - 1, per, width), bf16),
            pltpu.VMEM((n // 2, per, width), bf16),
            pltpu.VMEM((per, width), bf16),
            pltpu.VMEM((per, width), bf16),
            pltpu.VMEM((maps, cols_here), bf16),
            pltpu.VMEM((2, maps, 2 * TILE), bf16),
            pltpu.VMEM((maps, TILE), bf16),
            pltpu.VMEM((2, maps, TILE), f32),
            pltpu.VMEM((maps, LANES), f32),
            pltpu.VMEM((L, maps), f32),
            pltpu.VMEM((n_rows - 1, piece, maps), f32),
            pltpu.VMEM((piece, maps), f32),
            pltpu.VMEM((n, piece, maps), f32),
            pltpu.VMEM((piece, maps), f32),
            pltpu.SemaphoreType.DMA((8,)),
            plane, plane, half, pltpu.SemaphoreType.DMA, plane, pltpu.SemaphoreType.DMA((n,)),
            line, half, line, line, plane, plane, line, line,
        ],
        compiler_params=pltpu.CompilerParams(
            collective_id=1, has_side_effects=True, vmem_limit_bytes=50 * 2**20
        ),
        name="qml",
    )(*[pltpu.with_memory_space_constraint(value, pltpu.HBM) for value in inputs])
    return filtered.T, spectra


def solution(mesh):
    in_specs = (P("prow", "pcol"), P("prow", "pcol"), P("pcol", None))
    out_specs = (P("prow", None), P())
    n_rows, n_cols = mesh.shape["prow"], mesh.shape["pcol"]

    def whole(inverse_cov, cosines, sky_maps):
        npix = cosines.shape[0]
        step = jax.shard_map(
            functools.partial(per_device, npix, n_rows, n_cols),
            mesh=mesh, in_specs=in_specs, out_specs=out_specs, check_vma=False,
        )
        return step(inverse_cov, cosines, sky_maps)

    return whole
```

```python
import functools
import math

import jax
import jax.numpy as jnp
import numpy as np
from jax import lax
from jax.experimental import pallas as pl
from jax.experimental.pallas import tpu as pltpu
from jax.sharding import PartitionSpec as P

L = 64
LMIN = 2
TOP = LMIN + L - 1
LEVELS = TOP + 1
UNROLL = 22
HALF = LEVELS // 2
SPARE_UNROLL = 33
TILE = 256
STRIP = 32
N_X = 4
PARTS = 2
LANES = 128
MESH = pl.DeviceIdType.MESH


def transform_matrix(npix):
    a = [math.comb(2 * k, k) / 4.0**k for k in range(TOP + 1)]
    out = np.zeros((-(-LEVELS // 8) * 8, LANES))
    for l in range(LMIN, TOP + 1):
        for k in range(l + 1):
            out[abs(l - 2 * k), l - LMIN] += a[k] * a[l - k] * (2 * l + 1) / npix
    return out.astype(np.float32)


def rank_order(rows, cols):
    spots = [(dz, dx) for dz in range(rows) for dx in range(cols) if dz or dx]
    reach = lambda d, n: min(d, n - d)
    return sorted(spots, key=lambda s: -(reach(s[0], rows) + reach(s[1], cols)))


LINE = [4, 5, 3, 2, 6, 1, 7]


def qml_kernel(
    n_rows, n_z, n_x,
    sky_hbm, cov_hbm, cos_hbm, matrix_hbm,
    rows, spectra_out,
    sky, cov, cos, matrix, cheb, cheb_x, part, parcel, landed, rest, landed_rest, mine, cols,
    lhs, lhs_x, rows_x, fj, total, share, line_landed, line_sum, plane_landed, result,
    load_sem, send1, recv1, send_rest, recv_rest, send2, recv2, send3, recv3,
    send4, recv4, send5, recv5, send6, recv6, send_x, recv_x,
):
    r = lax.axis_index("prow")
    c = lax.axis_index("pcol")
    n = n_z * n_x
    z, x = c // n_x, lax.rem(c, n_x)
    q, h = c // 2, lax.rem(c, 2)
    half_n = n // 2
    maps = sky.shape[0]
    per, width = parcel.shape[1], parcel.shape[2]
    order = rank_order(n_z, n_x)
    diagonal = r == q
    off = r != q
    partner = r + 1 - 2 * lax.rem(r, 2)
    helper = partner == q
    side = jnp.where(r > q, h, 1 - h)
    barrier = pltpu.get_barrier_semaphore()

    def peer(spot):
        return lax.rem(z + spot[0], n_z) * n_x + lax.rem(x + spot[1], n_x)

    def line(e):
        return lax.rem(r + e, n_rows)

    def turn(row):
        return n_x // 2 * lax.rem(row, 2) + n_x - 1

    def chunk_of(row, col):
        return lax.rem(lax.rem(col, n_x) - turn(row) + 2 * n_x, n_x) * n_z + col // n_x

    def owner(row, k):
        return (k % n_z if isinstance(k, int) else lax.rem(k, n_z)) * n_x + lax.rem(k // n_z + turn(row), n_x)

    me = chunk_of(r, c)

    def signal(device):
        pl.semaphore_signal(barrier, inc=1, device_id=device, device_id_type=MESH)

    def copy(src, dst, send, recv, device):
        return pltpu.make_async_remote_copy(
            src_ref=src, dst_ref=dst, send_sem=send, recv_sem=recv,
            device_id=device, device_id_type=MESH,
        )

    first = [jnp.where(diagonal, 2 * h, 2 * side), jnp.where(diagonal, 1 + 2 * h, 2 * side)]
    second = [jnp.where(diagonal, 2 * h + 1, 2 * side + 1), jnp.where(diagonal, 2 - 2 * h, 2 * side + 1)]
    spare = 2 - h

    def tile_at(index):
        return pl.ds(pl.multiple_of(index * TILE, TILE), TILE)

    loads = [
        pltpu.make_async_copy(sky_hbm, sky, load_sem.at[0]),
        pltpu.make_async_copy(cov_hbm, cov, load_sem.at[1]),
    ]
    for t in range(2):
        for s, row in enumerate((first[t], second[t])):
            loads.append(
                pltpu.make_async_copy(
                    cos_hbm.at[tile_at(row), pl.ds(t * TILE, TILE)],
                    cos.at[pl.ds((2 * t + s) * TILE, TILE)],
                    load_sem.at[2 + 2 * t + s],
                )
            )
    matrix_load = pltpu.make_async_copy(matrix_hbm, matrix, load_sem.at[7])
    spare_load = pltpu.make_async_copy(
        cos_hbm.at[tile_at(spare), tile_at(h)], cos.at[pl.ds(4 * TILE, TILE)], load_sem.at[6]
    )
    for load in loads[:2]:
        load.start()

    for spot in order:
        signal((r, peer(spot)))
    for e in LINE:
        signal((line(e), c))

    @pl.when(off)
    def _():
        for j in range(half_n):
            signal((q, owner(q, h * half_n + j)))

    loads[0].wait()
    loads[1].wait()
    for load in loads[2:]:
        load.start()
    matrix_load.start()

    @pl.when(diagonal)
    def _():
        spare_load.start()

    wide = 2 * width
    for g in range(cov.shape[0] // wide):
        value = lax.dot_general(
            sky[...], cov[g * wide : (g + 1) * wide, :], (((1,), (1,)), ((), ())),
            preferred_element_type=jnp.float32,
        )
        for a in range(2):
            for b in range(maps // per):
                k = (2 * g + a) * (maps // per) + b
                piece = value[b * per : (b + 1) * per, a * width : (a + 1) * width]
                part[k] = piece
                parcel[k] = piece.astype(jnp.bfloat16)

    pl.semaphore_wait(barrier, len(order) + 2 * (n_rows - 1))

    def part_of(ref, p):
        return ref.at[pl.ds(p * (per // PARTS), per // PARTS)]

    def scatter(s, p):
        to = peer(order[s])
        return copy(
            part_of(parcel.at[chunk_of(r, to)], p), part_of(landed.at[s], p),
            send1.at[s], recv1.at[PARTS * s + p], (r, to),
        )

    def scatter_rest(j, p):
        to = owner(r, h * half_n + j)
        return copy(part_of(rest.at[j], p), part_of(landed_rest, p), send_rest.at[j], recv_rest.at[p], (r, to))

    def spare_cos():
        tile = cos.at[pl.ds(4 * TILE, TILE)]
        return copy(tile, tile, send_x.at[0], recv_x.at[0], (partner, c))

    def spare_rows():
        return copy(rows.at[:, tile_at(spare)], rows_x, send_x.at[1], recv_x.at[1], (partner, c))

    for s in range(len(order)):
        scatter(s, 0).start()

    @pl.when(diagonal)
    def _():
        for j in range(half_n):
            k = h * half_n + j
            rest[j] = (part[k] - parcel[k].astype(jnp.float32)).astype(jnp.bfloat16)

    for p in range(PARTS):
        @pl.when(diagonal)
        def _():
            for j in range(half_n):
                @pl.when(me != h * half_n + j)
                def _():
                    scatter_rest(j, p).start()

        if p + 1 < PARTS:
            for s in range(len(order)):
                scatter(s, p + 1).start()

    def generate(base, store, count=LEVELS):
        def strip(s, carry):
            at = pl.multiple_of(s * STRIP, STRIP)
            value = cos[pl.ds(base + at, STRIP), :]
            double = value + value
            before, now = value, jnp.ones_like(value)
            for k in range(count):
                store(k, at, now.astype(jnp.bfloat16))
                before, now = now, double * now - before
            return carry

        return strip

    def generate_pair(t):
        def store(k, at, value):
            cheb[k, t, pl.ds(at, STRIP), :] = value

        loads[2 + 2 * t].wait()
        loads[3 + 2 * t].wait()
        lax.fori_loop(0, 2 * TILE // STRIP, generate(2 * t * TILE, store), 0)

    @pl.when(diagonal)
    def _():
        spare_load.wait()
        spare_cos().start()

    generate_pair(0)

    chunk_half = me // half_n
    has_rest = c != 2 * r + chunk_half

    def place(ref, k):
        return ref.at[
            pl.ds(pl.multiple_of(lax.rem(k, 2) * per, per), per),
            pl.ds(pl.multiple_of((k // 2) * width, width), width),
        ]

    def gather(s, cut=lambda ref: ref):
        return copy(cut(mine), cut(place(rows, me)), send2.at[s], recv2.at[me], (r, peer(order[s])))

    def gathered(k):
        return copy(mine, place(rows, k), send2.at[0], recv2.at[k], (r, owner(r, k)))

    def column(e, cut=lambda ref: ref):
        return copy(
            cut(mine), cut(place(cols, lax.rem(me, half_n))), send3.at[e - 1], recv3.at[lax.rem(me, half_n)],
            (line(e), 2 * r + chunk_half),
        )

    def wanted(to):
        parity = jnp.where(to // 2 < r, chunk_half, 1 - chunk_half)
        return jnp.logical_or(to // 2 == r, lax.rem(to, 2) == parity)

    for p in range(PARTS):
        cut = functools.partial(part_of, p=p)
        span = slice(p * (per // PARTS), (p + 1) * (per // PARTS))
        sum_value = part[me, span]
        for s in range(len(order)):
            scatter(s, p).wait_recv()
            sum_value = sum_value + landed[s, span].astype(jnp.float32)
        part[me, span] = sum_value

        @pl.when(has_rest)
        def _():
            copy(
                part_of(rest.at[0], p), part_of(landed_rest, p), send_rest.at[0], recv_rest.at[p],
                (r, 2 * r + chunk_half),
            ).wait_recv()
            part[me, span] = part[me, span] + landed_rest[span].astype(jnp.float32)

        mine[span] = part[me, span].astype(jnp.bfloat16)
        for e in LINE[:4]:
            column(e, cut).start()
        for s in range(len(order)):
            @pl.when(wanted(peer(order[s])))
            def _():
                gather(s, cut).start()
        for e in LINE[4:]:
            column(e, cut).start()
    rows[
        pl.ds(pl.multiple_of(lax.rem(me, 2) * per, per), per),
        pl.ds(pl.multiple_of((me // 2) * width, width), width),
    ] = mine[...]

    generate_pair(1)

    @pl.when(diagonal)
    def _():
        def store(k, at, value):
            if k >= HALF:
                cheb_x[k - HALF, pl.ds(at, STRIP), :] = value

        lax.fori_loop(0, TILE // STRIP, generate(4 * TILE, store), 0)

    @pl.when(helper)
    def _():
        def store(k, at, value):
            cheb_x[k, pl.ds(at, STRIP), :] = value

        spare_cos().wait_recv()
        lax.fori_loop(0, TILE // STRIP, generate(4 * TILE, store, HALF), 0)

    for s in range(len(order)):
        @pl.when(jnp.logical_not(wanted(peer(order[s]))))
        def _():
            gather(s).start()

    for k in range(n):
        needed = jnp.logical_or(diagonal, side == k // half_n)

        @pl.when(jnp.logical_and(needed, me != k))
        def _():
            gathered(k).wait_recv()

    @pl.when(off)
    def _():
        for j in range(half_n):
            copy(
                mine, place(cols, j), send3.at[0], recv3.at[j], (q, owner(q, h * half_n + j))
            ).wait_recv()

    @pl.when(diagonal)
    def _():
        spare_rows().start()
        size = cols.shape[1]
        cols[...] = rows[:, pl.ds(pl.multiple_of(h * size, size), size)]

    weight = jnp.where(diagonal, 1, 2).astype(jnp.float32)
    for t in range(2):
        lhs[t, :, :TILE] = (rows[:, tile_at(first[t])].astype(jnp.float32) * weight).astype(jnp.bfloat16)
        lhs[t, :, TILE:] = (rows[:, tile_at(second[t])].astype(jnp.float32) * 2.0).astype(jnp.bfloat16)
        fj[t] = cols[:, t * TILE : (t + 1) * TILE].astype(jnp.float32)

    matrix_load.wait()
    total[...] = jnp.zeros_like(total)

    def add_moment(acc, prod, k):
        narrow = prod[:, :LANES] + prod[:, LANES:]
        return acc + jnp.sum(narrow, axis=-1, keepdims=True) * matrix[pl.ds(k, 1), :]

    def level_step(step, carry):
        acc = total[...]
        for u in range(UNROLL):
            k = step * UNROLL + u
            prod = None
            for t in range(2):
                image = jnp.dot(lhs[t], cheb[k, t], preferred_element_type=jnp.float32)
                term = image * fj[t]
                prod = term if prod is None else prod + term
            acc = add_moment(acc, prod, k)
        total[...] = acc
        return carry

    lax.fori_loop(0, LEVELS // UNROLL, level_step, 0)

    @pl.when(diagonal)
    def _():
        lhs_x[...] = (rows[:, tile_at(spare)].astype(jnp.float32) * 2.0).astype(jnp.bfloat16)

    @pl.when(helper)
    def _():
        spare_rows().wait_recv()
        lhs_x[...] = (rows_x[...].astype(jnp.float32) * 2.0).astype(jnp.bfloat16)

    @pl.when(jnp.logical_or(diagonal, helper))
    def _():
        base = jnp.where(diagonal, HALF, 0)

        def spare_step(step, carry):
            acc = total[...]
            for u in range(SPARE_UNROLL):
                k = step * SPARE_UNROLL + u
                image = jnp.dot(lhs_x[...], cheb_x[k], preferred_element_type=jnp.float32)
                acc = add_moment(acc, image * fj[h], base + k)
            total[...] = acc
            return carry

        lax.fori_loop(0, HALF // SPARE_UNROLL, spare_step, 0)

    share[...] = total[...].T[:L]

    piece = L // n_rows

    def block(k):
        return pl.ds(pl.multiple_of(k * piece, piece), piece)

    def reduce_line(e):
        return copy(
            share.at[block(line(e))], line_landed.at[e - 1], send4.at[e - 1], recv4.at[e - 1], (line(e), c)
        )

    def exchange(s):
        return copy(line_sum, plane_landed.at[c], send5.at[s], recv5.at[s], (r, peer(order[s])))

    def spread_line(e, k):
        return copy(result, spectra_out.at[block(k)], send6.at[e - 1], recv6.at[e - 1], (line(e), c))

    for e in LINE:
        reduce_line(e).start()

    for k in range(n):
        needed = jnp.logical_or(diagonal, side == k // half_n)

        @pl.when(jnp.logical_and(jnp.logical_not(needed), me != k))
        def _():
            gathered(k).wait_recv()

    for e in LINE:
        reduce_line(e).wait_recv()
    value = share[block(r)]
    for e in range(1, n_rows):
        value = value + line_landed[e - 1]
    line_sum[...] = value
    for s in range(len(order)):
        exchange(s).start()
    plane_landed[c] = value
    for s in range(len(order)):
        exchange(s).wait_recv()
    value = plane_landed[0]
    for k in range(1, n):
        value = value + plane_landed[k]
    result[...] = value
    for e in LINE:
        spread_line(e, r).start()
    spectra_out[block(r)] = value
    for e in LINE:
        spread_line(e, lax.rem(r - e + n_rows, n_rows)).wait_recv()

    for s in range(len(order)):
        copy(parcel.at[0], landed.at[s], send1.at[s], recv1.at[s], (r, peer(order[s]))).wait_send()
        gather(s).wait_send()
        exchange(s).wait_send()
    for e in LINE:
        column(e).wait_send()
        reduce_line(e).wait_send()
        spread_line(e, r).wait_send()

    @pl.when(diagonal)
    def _():
        spare_cos().wait_send()
        spare_rows().wait_send()
        for j in range(half_n):
            @pl.when(me != h * half_n + j)
            def _():
                copy(rest.at[j], landed_rest, send_rest.at[j], recv_rest.at[0], (r, c)).wait_send()


def close_kernel(filtered, spectra, filtered_out, spectra_out, sem):
    copies = [
        pltpu.make_async_copy(filtered, filtered_out, sem.at[0]),
        pltpu.make_async_copy(spectra, spectra_out, sem.at[1]),
    ]
    for copy in copies:
        copy.start()
    for copy in copies:
        copy.wait()


def per_device(npix, n_rows, n_cols, inverse_cov, cosines, sky_maps):
    n_z = n_cols // N_X
    n = n_cols
    size, cols_here = inverse_cov.shape
    maps = sky_maps.shape[1]
    sky_t = sky_maps.T
    per, width = maps // 2, 2 * size // n
    piece = L // n_rows
    vmem = pl.BlockSpec(memory_space=pltpu.VMEM)
    hbm = pl.BlockSpec(memory_space=pltpu.HBM)
    matrix = jnp.asarray(transform_matrix(npix))
    inputs = (sky_t, inverse_cov, cosines, matrix)
    bf16, f32 = jnp.bfloat16, jnp.float32
    plane = pltpu.SemaphoreType.DMA((n - 1,))
    line = pltpu.SemaphoreType.DMA((n_rows - 1,))
    half = pltpu.SemaphoreType.DMA((n // 2,))
    filtered, spectra = pl.pallas_call(
        functools.partial(qml_kernel, n_rows, n_z, N_X),
        out_shape=(
            jax.ShapeDtypeStruct((maps, size), bf16),
            jax.ShapeDtypeStruct((L, maps), f32),
        ),
        in_specs=[hbm] * len(inputs),
        out_specs=(vmem, vmem),
        scratch_shapes=[
            pltpu.VMEM(sky_t.shape, bf16),
            pltpu.VMEM(inverse_cov.shape, bf16),
            pltpu.VMEM((5 * TILE, TILE), f32),
            pltpu.VMEM(matrix.shape, f32),
            pltpu.VMEM((LEVELS, 2, 2 * TILE, TILE), bf16),
            pltpu.VMEM((HALF, TILE, TILE), bf16),
            pltpu.VMEM((n, per, width), f32),
            pltpu.VMEM((n, per, width), bf16),
            pltpu.VMEM((n - 1, per, width), bf16),
            pltpu.VMEM((n // 2, per, width), bf16),
            pltpu.VMEM((per, width), bf16),
            pltpu.VMEM((per, width), bf16),
            pltpu.VMEM((maps, cols_here), bf16),
            pltpu.VMEM((2, maps, 2 * TILE), bf16),
            pltpu.VMEM((maps, TILE), bf16),
            pltpu.VMEM((maps, TILE), bf16),
            pltpu.VMEM((2, maps, TILE), f32),
            pltpu.VMEM((maps, LANES), f32),
            pltpu.VMEM((L, maps), f32),
            pltpu.VMEM((n_rows - 1, piece, maps), f32),
            pltpu.VMEM((piece, maps), f32),
            pltpu.VMEM((n, piece, maps), f32),
            pltpu.VMEM((piece, maps), f32),
            pltpu.SemaphoreType.DMA((8,)),
            plane, pltpu.SemaphoreType.DMA((PARTS * (n - 1),)), half, pltpu.SemaphoreType.DMA((PARTS,)),
            plane, pltpu.SemaphoreType.DMA((n,)),
            line, half, line, line, plane, plane, line, line,
            pltpu.SemaphoreType.DMA((2,)), pltpu.SemaphoreType.DMA((2,)),
        ],
        compiler_params=pltpu.CompilerParams(
            collective_id=1, has_side_effects=True, vmem_limit_bytes=50 * 2**20
        ),
        name="qml",
    )(*[pltpu.with_memory_space_constraint(value, pltpu.HBM) for value in inputs])
    filtered, spectra = pl.pallas_call(
        close_kernel,
        out_shape=(pltpu.HBM(filtered.shape, bf16), pltpu.HBM(spectra.shape, f32)),
        in_specs=[vmem, vmem],
        out_specs=(hbm, hbm),
        scratch_shapes=[pltpu.SemaphoreType.DMA((2,))],
        compiler_params=pltpu.CompilerParams(vmem_limit_bytes=2**20),
        name="close",
    )(filtered, spectra)
    return filtered.T, spectra


def solution(mesh):
    in_specs = (P("prow", "pcol"), P("prow", "pcol"), P("pcol", None))
    out_specs = (P("prow", None), P())
    n_rows, n_cols = mesh.shape["prow"], mesh.shape["pcol"]

    def whole(inverse_cov, cosines, sky_maps):
        npix = cosines.shape[0]
        step = jax.shard_map(
            functools.partial(per_device, npix, n_rows, n_cols),
            mesh=mesh, in_specs=in_specs, out_specs=out_specs, check_vma=False,
        )
        return step(inverse_cov, cosines, sky_maps)

    return whole
```

```python
import functools
import math

import jax
import jax.numpy as jnp
import numpy as np
from jax import lax
from jax.experimental import pallas as pl
from jax.experimental.pallas import tpu as pltpu
from jax.sharding import PartitionSpec as P

L = 64
LMIN = 2
TOP = LMIN + L - 1
LEVELS = TOP + 1
UNROLL = 22
HALF = LEVELS // 2
SPARE_UNROLL = 33
TILE = 256
STRIP = 32
N_X = 4
PARTS = 2
LANES = 128
MESH = pl.DeviceIdType.MESH


def transform_matrix(npix):
    a = [math.comb(2 * k, k) / 4.0**k for k in range(TOP + 1)]
    out = np.zeros((-(-LEVELS // 8) * 8, LANES))
    for l in range(LMIN, TOP + 1):
        for k in range(l + 1):
            out[abs(l - 2 * k), l - LMIN] += a[k] * a[l - k] * (2 * l + 1) / npix
    return out.astype(np.float32)


def rank_order(rows, cols):
    spots = [(dz, dx) for dz in range(rows) for dx in range(cols) if dz or dx]
    reach = lambda d, n: min(d, n - d)
    return sorted(spots, key=lambda s: -(reach(s[0], rows) + reach(s[1], cols)))


LINE = [4, 5, 3, 2, 6, 1, 7]


def qml_kernel(
    n_rows, n_z, n_x,
    sky_hbm, cov_hbm, cos_hbm, matrix_hbm,
    rows, spectra_out,
    sky, cov, cos, matrix, cheb, cheb_x, part, parcel, landed, rest, landed_rest, mine, cols,
    lhs, lhs_x, rows_x, fj, total, share, line_landed, line_sum, plane_landed, result,
    load_sem, send1, recv1, send_rest, recv_rest, send2, recv2, send3, recv3,
    send4, recv4, send5, recv5, send6, recv6, send_x, recv_x,
):
    r = lax.axis_index("prow")
    c = lax.axis_index("pcol")
    n = n_z * n_x
    z, x = c // n_x, lax.rem(c, n_x)
    q, h = c // 2, lax.rem(c, 2)
    half_n = n // 2
    maps = sky.shape[0]
    per, width = parcel.shape[1], parcel.shape[2]
    order = rank_order(n_z, n_x)
    diagonal = r == q
    off = r != q
    partner = r + 1 - 2 * lax.rem(r, 2)
    helper = partner == q
    lead = lax.rem(r, 2) == 1
    side = jnp.where(r > q, h, 1 - h)
    barrier = pltpu.get_barrier_semaphore()

    def peer(spot):
        return lax.rem(z + spot[0], n_z) * n_x + lax.rem(x + spot[1], n_x)

    def line(e):
        return lax.rem(r + e, n_rows)

    def turn(row):
        return n_x // 2 * lax.rem(row, 2) + n_x - 1

    def chunk_of(row, col):
        return lax.rem(lax.rem(col, n_x) - turn(row) + 2 * n_x, n_x) * n_z + col // n_x

    def owner(row, k):
        return (k % n_z if isinstance(k, int) else lax.rem(k, n_z)) * n_x + lax.rem(k // n_z + turn(row), n_x)

    me = chunk_of(r, c)

    def signal(device):
        pl.semaphore_signal(barrier, inc=1, device_id=device, device_id_type=MESH)

    def copy(src, dst, send, recv, device):
        return pltpu.make_async_remote_copy(
            src_ref=src, dst_ref=dst, send_sem=send, recv_sem=recv,
            device_id=device, device_id_type=MESH,
        )

    first = [jnp.where(diagonal, 2 * h, 2 * side), jnp.where(diagonal, 1 + 2 * h, 2 * side)]
    second = [jnp.where(diagonal, 2 * h + 1, 2 * side + 1), jnp.where(diagonal, 2 - 2 * h, 2 * side + 1)]
    spare = 2 - h

    def tile_at(index):
        return pl.ds(pl.multiple_of(index * TILE, TILE), TILE)

    loads = [
        pltpu.make_async_copy(sky_hbm, sky, load_sem.at[0]),
        pltpu.make_async_copy(cov_hbm, cov, load_sem.at[1]),
    ]
    for t in range(2):
        for s, row in enumerate((first[t], second[t])):
            loads.append(
                pltpu.make_async_copy(
                    cos_hbm.at[tile_at(row), pl.ds(t * TILE, TILE)],
                    cos.at[pl.ds((2 * t + s) * TILE, TILE)],
                    load_sem.at[2 + 2 * t + s],
                )
            )
    matrix_load = pltpu.make_async_copy(matrix_hbm, matrix, load_sem.at[7])
    spare_load = pltpu.make_async_copy(
        cos_hbm.at[tile_at(spare), tile_at(h)], cos.at[pl.ds(4 * TILE, TILE)], load_sem.at[6]
    )
    for load in loads[:2]:
        load.start()

    for spot in order:
        signal((r, peer(spot)))
    for e in LINE:
        signal((line(e), c))

    @pl.when(off)
    def _():
        for j in range(half_n):
            signal((q, owner(q, h * half_n + j)))

    loads[0].wait()
    loads[1].wait()
    for load in loads[2:]:
        load.start()
    matrix_load.start()

    @pl.when(diagonal)
    def _():
        spare_load.start()

    wide = 2 * width
    for g in range(cov.shape[0] // wide):
        value = lax.dot_general(
            sky[...], cov[g * wide : (g + 1) * wide, :], (((1,), (1,)), ((), ())),
            preferred_element_type=jnp.float32,
        )
        for a in range(2):
            for b in range(maps // per):
                k = (2 * g + a) * (maps // per) + b
                piece = value[b * per : (b + 1) * per, a * width : (a + 1) * width]
                part[k] = piece
                parcel[k] = piece.astype(jnp.bfloat16)

    pl.semaphore_wait(barrier, len(order) + 2 * (n_rows - 1))

    def part_of(ref, p):
        return ref.at[pl.ds(p * (per // PARTS), per // PARTS)]

    def scatter(s, p):
        to = peer(order[s])
        return copy(
            part_of(parcel.at[chunk_of(r, to)], p), part_of(landed.at[s], p),
            send1.at[s], recv1.at[PARTS * s + p], (r, to),
        )

    def scatter_rest(j, p):
        to = owner(r, h * half_n + j)
        return copy(part_of(rest.at[j], p), part_of(landed_rest, p), send_rest.at[j], recv_rest.at[p], (r, to))

    def spare_cos():
        tile = cos.at[pl.ds(4 * TILE, TILE)]
        return copy(tile, tile, send_x.at[0], recv_x.at[0], (partner, c))

    def spare_rows():
        return copy(rows.at[:, tile_at(spare)], rows_x, send_x.at[1], recv_x.at[1], (partner, c))

    for s in range(len(order)):
        scatter(s, 0).start()

    @pl.when(diagonal)
    def _():
        for j in range(half_n):
            k = h * half_n + j
            rest[j] = (part[k] - parcel[k].astype(jnp.float32)).astype(jnp.bfloat16)

    for p in range(PARTS):
        @pl.when(diagonal)
        def _():
            for j in range(half_n):
                @pl.when(me != h * half_n + j)
                def _():
                    scatter_rest(j, p).start()

        if p + 1 < PARTS:
            for s in range(len(order)):
                scatter(s, p + 1).start()

    def generate(base, store, count=LEVELS):
        def strip(s, carry):
            at = pl.multiple_of(s * STRIP, STRIP)
            value = cos[pl.ds(base + at, STRIP), :]
            double = value + value
            before, now = value, jnp.ones_like(value)
            for k in range(count):
                store(k, at, now.astype(jnp.bfloat16))
                before, now = now, double * now - before
            return carry

        return strip

    def generate_pair(t):
        def store(k, at, value):
            cheb[k, t, pl.ds(at, STRIP), :] = value

        loads[2 + 2 * t].wait()
        loads[3 + 2 * t].wait()
        lax.fori_loop(0, 2 * TILE // STRIP, generate(2 * t * TILE, store), 0)

    @pl.when(diagonal)
    def _():
        spare_load.wait()
        spare_cos().start()

    generate_pair(0)

    @pl.when(diagonal)
    def _():
        def store(k, at, value):
            if k >= HALF:
                cheb_x[k - HALF, pl.ds(at, STRIP), :] = value

        lax.fori_loop(0, TILE // STRIP, generate(4 * TILE, store), 0)


    chunk_half = me // half_n
    has_rest = c != 2 * r + chunk_half

    def place(ref, k):
        return ref.at[
            pl.ds(pl.multiple_of(lax.rem(k, 2) * per, per), per),
            pl.ds(pl.multiple_of((k // 2) * width, width), width),
        ]

    def gather(s, cut=lambda ref: ref):
        return copy(cut(mine), cut(place(rows, me)), send2.at[s], recv2.at[me], (r, peer(order[s])))

    def gathered(k):
        return copy(mine, place(rows, k), send2.at[0], recv2.at[k], (r, owner(r, k)))

    def column(e, cut=lambda ref: ref):
        return copy(
            cut(mine), cut(place(cols, lax.rem(me, half_n))), send3.at[e - 1], recv3.at[lax.rem(me, half_n)],
            (line(e), 2 * r + chunk_half),
        )

    def wanted(to):
        parity = jnp.where(to // 2 < r, chunk_half, 1 - chunk_half)
        return jnp.logical_or(to // 2 == r, lax.rem(to, 2) == parity)

    for p in range(PARTS):
        cut = functools.partial(part_of, p=p)
        span = slice(p * (per // PARTS), (p + 1) * (per // PARTS))
        sum_value = part[me, span]
        for s in range(len(order)):
            scatter(s, p).wait_recv()
            sum_value = sum_value + landed[s, span].astype(jnp.float32)
        part[me, span] = sum_value

        @pl.when(has_rest)
        def _():
            copy(
                part_of(rest.at[0], p), part_of(landed_rest, p), send_rest.at[0], recv_rest.at[p],
                (r, 2 * r + chunk_half),
            ).wait_recv()
            part[me, span] = part[me, span] + landed_rest[span].astype(jnp.float32)

        mine[span] = part[me, span].astype(jnp.bfloat16)
        for e in LINE[:4]:
            column(e, cut).start()
        for s in range(len(order)):
            @pl.when(wanted(peer(order[s])))
            def _():
                gather(s, cut).start()
        for e in LINE[4:]:
            column(e, cut).start()
    rows[
        pl.ds(pl.multiple_of(lax.rem(me, 2) * per, per), per),
        pl.ds(pl.multiple_of((me // 2) * width, width), width),
    ] = mine[...]

    generate_pair(1)

    @pl.when(helper)
    def _():
        def store(k, at, value):
            cheb_x[k, pl.ds(at, STRIP), :] = value

        spare_cos().wait_recv()
        lax.fori_loop(0, TILE // STRIP, generate(4 * TILE, store, HALF), 0)

    for s in range(len(order)):
        @pl.when(jnp.logical_not(wanted(peer(order[s]))))
        def _():
            gather(s).start()

    for k in range(n):
        needed = jnp.logical_or(diagonal, side == k // half_n)

        @pl.when(jnp.logical_and(needed, me != k))
        def _():
            gathered(k).wait_recv()

    @pl.when(off)
    def _():
        for j in range(half_n):
            copy(
                mine, place(cols, j), send3.at[0], recv3.at[j], (q, owner(q, h * half_n + j))
            ).wait_recv()

    @pl.when(diagonal)
    def _():
        spare_rows().start()
        size = cols.shape[1]
        cols[...] = rows[:, pl.ds(pl.multiple_of(h * size, size), size)]

    weight = jnp.where(diagonal, 1, 2).astype(jnp.float32)
    for t in range(2):
        lhs[t, :, :TILE] = (rows[:, tile_at(first[t])].astype(jnp.float32) * weight).astype(jnp.bfloat16)
        lhs[t, :, TILE:] = (rows[:, tile_at(second[t])].astype(jnp.float32) * 2.0).astype(jnp.bfloat16)
        fj[t] = cols[:, t * TILE : (t + 1) * TILE].astype(jnp.float32)

    matrix_load.wait()
    total[...] = jnp.zeros_like(total)

    def add_moment(acc, prod, k):
        narrow = prod[:, :LANES] + prod[:, LANES:]
        return acc + jnp.sum(narrow, axis=-1, keepdims=True) * matrix[pl.ds(k, 1), :]

    def level_step(step, carry):
        acc = total[...]
        for u in range(UNROLL):
            k = step * UNROLL + u
            prod = None
            for t in range(2):
                image = jnp.dot(lhs[t], cheb[k, t], preferred_element_type=jnp.float32)
                term = image * fj[t]
                prod = term if prod is None else prod + term
            acc = add_moment(acc, prod, k)
        total[...] = acc
        return carry

    lax.fori_loop(0, LEVELS // UNROLL, level_step, 0)

    @pl.when(diagonal)
    def _():
        lhs_x[...] = (rows[:, tile_at(spare)].astype(jnp.float32) * 2.0).astype(jnp.bfloat16)

    @pl.when(helper)
    def _():
        spare_rows().wait_recv()
        lhs_x[...] = (rows_x[...].astype(jnp.float32) * 2.0).astype(jnp.bfloat16)

    @pl.when(jnp.logical_or(diagonal, helper))
    def _():
        base = jnp.where(diagonal, HALF, 0)

        def spare_step(step, carry):
            acc = total[...]
            for u in range(SPARE_UNROLL):
                k = step * SPARE_UNROLL + u
                image = jnp.dot(lhs_x[...], cheb_x[k], preferred_element_type=jnp.float32)
                acc = add_moment(acc, image * fj[h], base + k)
            total[...] = acc
            return carry

        lax.fori_loop(0, HALF // SPARE_UNROLL, spare_step, 0)

    share[...] = total[...].T[:L]

    chips = n_rows // 2
    piece = L // chips
    core, y = lax.rem(r, 2), r // 2

    def block(k):
        return pl.ds(pl.multiple_of(k * piece, piece), piece)

    def across(d):
        return lax.rem(y + d, chips)

    def reduce_line(d, source=core):
        k = across(d)
        return copy(
            share.at[block(k)], line_landed.at[2 * d + source], send4.at[d], recv4.at[2 * d + source],
            (2 * k + 1, c),
        )

    def exchange(s):
        return copy(line_sum, plane_landed.at[c], send5.at[s], recv5.at[s], (r, peer(order[s])))

    def spread_line(d, target, k):
        return copy(
            result, spectra_out.at[block(k)], send6.at[2 * d + target], recv6.at[d], (2 * across(d) + target, c)
        )

    def finish_rows():
        for k in range(n):
            needed = jnp.logical_or(diagonal, side == k // half_n)

            @pl.when(jnp.logical_and(jnp.logical_not(needed), me != k))
            def _():
                gathered(k).wait_recv()

    for d in (2, 3, 1):
        reduce_line(d).start()

    @pl.when(jnp.logical_not(lead))
    def _():
        reduce_line(0, 0).start()

    finish_rows()

    @pl.when(lead)
    def _():
        value = share[block(y)]
        for d, source in ((0, 0), (1, 0), (1, 1), (3, 0), (3, 1), (2, 0), (2, 1)):
            reduce_line(d, source).wait_recv()
            value = value + line_landed[2 * d + source]
        line_sum[...] = value
        for s in range(len(order)):
            exchange(s).start()
        plane_landed[c] = value
        for s in range(len(order)):
            exchange(s).wait_recv()
        value = plane_landed[0]
        for k in range(1, n):
            value = value + plane_landed[k]
        result[...] = value
        for d in (2, 3, 1):
            for target in range(2):
                spread_line(d, target, y).start()
        spread_line(0, 0, y).start()
        spectra_out[block(y)] = value

    for d in (1, 3, 2):
        spread_line(d, 0, lax.rem(y - d + chips, chips)).wait_recv()

    @pl.when(jnp.logical_not(lead))
    def _():
        spread_line(0, 0, y).wait_recv()
        reduce_line(0, 0).wait_send()

    for d in (1, 2, 3):
        reduce_line(d).wait_send()

    @pl.when(lead)
    def _():
        for s in range(len(order)):
            exchange(s).wait_send()
        for d in (1, 2, 3):
            for target in range(2):
                spread_line(d, target, y).wait_send()
        spread_line(0, 0, y).wait_send()

    for s in range(len(order)):
        copy(parcel.at[0], landed.at[s], send1.at[s], recv1.at[s], (r, peer(order[s]))).wait_send()
        gather(s).wait_send()
    for e in LINE:
        column(e).wait_send()

    @pl.when(diagonal)
    def _():
        spare_cos().wait_send()
        spare_rows().wait_send()
        for j in range(half_n):
            @pl.when(me != h * half_n + j)
            def _():
                copy(rest.at[j], landed_rest, send_rest.at[j], recv_rest.at[0], (r, c)).wait_send()


def close_kernel(filtered, spectra, filtered_out, spectra_out, sem):
    copies = [
        pltpu.make_async_copy(filtered, filtered_out, sem.at[0]),
        pltpu.make_async_copy(spectra, spectra_out, sem.at[1]),
    ]
    for copy in copies:
        copy.start()
    for copy in copies:
        copy.wait()


def per_device(npix, n_rows, n_cols, inverse_cov, cosines, sky_maps):
    n_z = n_cols // N_X
    n = n_cols
    size, cols_here = inverse_cov.shape
    maps = sky_maps.shape[1]
    sky_t = sky_maps.T
    per, width = maps // 2, 2 * size // n
    piece = L // (n_rows // 2)
    vmem = pl.BlockSpec(memory_space=pltpu.VMEM)
    hbm = pl.BlockSpec(memory_space=pltpu.HBM)
    matrix = jnp.asarray(transform_matrix(npix))
    inputs = (sky_t, inverse_cov, cosines, matrix)
    bf16, f32 = jnp.bfloat16, jnp.float32
    plane = pltpu.SemaphoreType.DMA((n - 1,))
    line = pltpu.SemaphoreType.DMA((n_rows - 1,))
    half = pltpu.SemaphoreType.DMA((n // 2,))
    every = pltpu.SemaphoreType.DMA((n_rows,))
    filtered, spectra = pl.pallas_call(
        functools.partial(qml_kernel, n_rows, n_z, N_X),
        out_shape=(
            jax.ShapeDtypeStruct((maps, size), bf16),
            jax.ShapeDtypeStruct((L, maps), f32),
        ),
        in_specs=[hbm] * len(inputs),
        out_specs=(vmem, vmem),
        scratch_shapes=[
            pltpu.VMEM(sky_t.shape, bf16),
            pltpu.VMEM(inverse_cov.shape, bf16),
            pltpu.VMEM((5 * TILE, TILE), f32),
            pltpu.VMEM(matrix.shape, f32),
            pltpu.VMEM((LEVELS, 2, 2 * TILE, TILE), bf16),
            pltpu.VMEM((HALF, TILE, TILE), bf16),
            pltpu.VMEM((n, per, width), f32),
            pltpu.VMEM((n, per, width), bf16),
            pltpu.VMEM((n - 1, per, width), bf16),
            pltpu.VMEM((n // 2, per, width), bf16),
            pltpu.VMEM((per, width), bf16),
            pltpu.VMEM((per, width), bf16),
            pltpu.VMEM((maps, cols_here), bf16),
            pltpu.VMEM((2, maps, 2 * TILE), bf16),
            pltpu.VMEM((maps, TILE), bf16),
            pltpu.VMEM((maps, TILE), bf16),
            pltpu.VMEM((2, maps, TILE), f32),
            pltpu.VMEM((maps, LANES), f32),
            pltpu.VMEM((L, maps), f32),
            pltpu.VMEM((n_rows, piece, maps), f32),
            pltpu.VMEM((piece, maps), f32),
            pltpu.VMEM((n, piece, maps), f32),
            pltpu.VMEM((piece, maps), f32),
            pltpu.SemaphoreType.DMA((8,)),
            plane, pltpu.SemaphoreType.DMA((PARTS * (n - 1),)), half, pltpu.SemaphoreType.DMA((PARTS,)),
            plane, pltpu.SemaphoreType.DMA((n,)),
            line, half, line, every, plane, plane, every, line,
            pltpu.SemaphoreType.DMA((2,)), pltpu.SemaphoreType.DMA((2,)),
        ],
        compiler_params=pltpu.CompilerParams(
            collective_id=1, has_side_effects=True, vmem_limit_bytes=50 * 2**20
        ),
        name="qml",
    )(*[pltpu.with_memory_space_constraint(value, pltpu.HBM) for value in inputs])
    filtered, spectra = pl.pallas_call(
        close_kernel,
        out_shape=(pltpu.HBM(filtered.shape, bf16), pltpu.HBM(spectra.shape, f32)),
        in_specs=[vmem, vmem],
        out_specs=(hbm, hbm),
        scratch_shapes=[pltpu.SemaphoreType.DMA((2,))],
        compiler_params=pltpu.CompilerParams(vmem_limit_bytes=2**20),
        name="close",
    )(filtered, spectra)
    return filtered.T, spectra


def solution(mesh):
    in_specs = (P("prow", "pcol"), P("prow", "pcol"), P("pcol", None))
    out_specs = (P("prow", None), P())
    n_rows, n_cols = mesh.shape["prow"], mesh.shape["pcol"]

    def whole(inverse_cov, cosines, sky_maps):
        npix = cosines.shape[0]
        step = jax.shard_map(
            functools.partial(per_device, npix, n_rows, n_cols),
            mesh=mesh, in_specs=in_specs, out_specs=out_specs, check_vma=False,
        )
        return step(inverse_cov, cosines, sky_maps)

    return whole
```

```python
import functools
import math

import jax
import jax.numpy as jnp
import numpy as np
from jax import lax
from jax.experimental import pallas as pl
from jax.experimental.pallas import tpu as pltpu
from jax.sharding import PartitionSpec as P

L = 64
LMIN = 2
TOP = LMIN + L - 1
LEVELS = TOP + 1
UNROLL = 22
HALF = LEVELS // 2
SPARE_UNROLL = 33
TILE = 256
STRIP = 32
N_X = 4
PARTS = 2
LANES = 128
MESH = pl.DeviceIdType.MESH


def transform_matrix(npix):
    a = [math.comb(2 * k, k) / 4.0**k for k in range(TOP + 1)]
    out = np.zeros((-(-LEVELS // 8) * 8, LANES))
    for l in range(LMIN, TOP + 1):
        for k in range(l + 1):
            out[abs(l - 2 * k), l - LMIN] += a[k] * a[l - k] * (2 * l + 1) / npix
    return out.astype(np.float32)


def rank_order(rows, cols):
    spots = [(dz, dx) for dz in range(rows) for dx in range(cols) if dz or dx]
    reach = lambda d, n: min(d, n - d)
    return sorted(spots, key=lambda s: -(reach(s[0], rows) + reach(s[1], cols)))


LINE = [4, 5, 3, 2, 6, 1, 7]
SAME = [4, 2, 6]


def qml_kernel(
    n_rows, n_z, n_x,
    sky_hbm, cov_hbm, cos_hbm, matrix_hbm,
    rows, spectra_out,
    sky, cov, cos, matrix, cheb, cheb_x, part, parcel, landed, rest, landed_rest, mine, cols,
    lhs, lhs_x, rows_x, fj, total, share, line_landed, line_sum, plane_landed, result,
    load_sem, send1, recv1, send_rest, recv_rest, send2, recv2, send3, recv3,
    send4, recv4, send5, recv5, send6, recv6, send_x, recv_x, send_r,
):
    r = lax.axis_index("prow")
    c = lax.axis_index("pcol")
    n = n_z * n_x
    z, x = c // n_x, lax.rem(c, n_x)
    q, h = c // 2, lax.rem(c, 2)
    half_n = n // 2
    maps = sky.shape[0]
    per, width = parcel.shape[1], parcel.shape[2]
    order = rank_order(n_z, n_x)
    diagonal = r == q
    off = r != q
    partner = r + 1 - 2 * lax.rem(r, 2)
    helper = partner == q
    relays = lax.rem(r + q, 2) == 0
    relayed = lax.rem(r + q, 2) == 1
    lead = lax.rem(r, 2) == 1
    side = jnp.where(r > q, h, 1 - h)
    barrier = pltpu.get_barrier_semaphore()

    def peer(spot):
        return lax.rem(z + spot[0], n_z) * n_x + lax.rem(x + spot[1], n_x)

    def line(e):
        return lax.rem(r + e, n_rows)

    def turn(row):
        return n_x // 2 * lax.rem(row, 2) + n_x - 1

    def chunk_of(row, col):
        return lax.rem(lax.rem(col, n_x) - turn(row) + 2 * n_x, n_x) * n_z + col // n_x

    def owner(row, k):
        return (k % n_z if isinstance(k, int) else lax.rem(k, n_z)) * n_x + lax.rem(k // n_z + turn(row), n_x)

    me = chunk_of(r, c)

    def signal(device):
        pl.semaphore_signal(barrier, inc=1, device_id=device, device_id_type=MESH)

    def copy(src, dst, send, recv, device):
        return pltpu.make_async_remote_copy(
            src_ref=src, dst_ref=dst, send_sem=send, recv_sem=recv,
            device_id=device, device_id_type=MESH,
        )

    first = [jnp.where(diagonal, 2 * h, 2 * side), jnp.where(diagonal, 1 + 2 * h, 2 * side)]
    second = [jnp.where(diagonal, 2 * h + 1, 2 * side + 1), jnp.where(diagonal, 2 - 2 * h, 2 * side + 1)]
    spare = 2 - h

    def tile_at(index):
        return pl.ds(pl.multiple_of(index * TILE, TILE), TILE)

    loads = [
        pltpu.make_async_copy(sky_hbm, sky, load_sem.at[0]),
        pltpu.make_async_copy(cov_hbm, cov, load_sem.at[1]),
    ]
    for t in range(2):
        for s, row in enumerate((first[t], second[t])):
            loads.append(
                pltpu.make_async_copy(
                    cos_hbm.at[tile_at(row), pl.ds(t * TILE, TILE)],
                    cos.at[pl.ds((2 * t + s) * TILE, TILE)],
                    load_sem.at[2 + 2 * t + s],
                )
            )
    matrix_load = pltpu.make_async_copy(matrix_hbm, matrix, load_sem.at[7])
    spare_load = pltpu.make_async_copy(
        cos_hbm.at[tile_at(spare), tile_at(h)], cos.at[pl.ds(4 * TILE, TILE)], load_sem.at[6]
    )
    for load in loads[:2]:
        load.start()

    for spot in order:
        signal((r, peer(spot)))
    for e in LINE:
        signal((line(e), c))

    @pl.when(jnp.logical_and(off, relays))
    def _():
        for j in range(half_n):
            signal((q, owner(q, h * half_n + j)))

    loads[0].wait()
    loads[1].wait()
    for load in loads[2:]:
        load.start()
    matrix_load.start()

    @pl.when(diagonal)
    def _():
        spare_load.start()

    wide = 2 * width
    for g in range(cov.shape[0] // wide):
        value = lax.dot_general(
            sky[...], cov[g * wide : (g + 1) * wide, :], (((1,), (1,)), ((), ())),
            preferred_element_type=jnp.float32,
        )
        for a in range(2):
            for b in range(maps // per):
                k = (2 * g + a) * (maps // per) + b
                piece = value[b * per : (b + 1) * per, a * width : (a + 1) * width]
                part[k] = piece
                parcel[k] = piece.astype(jnp.bfloat16)

    pl.semaphore_wait(barrier, len(order) + len(LINE) + len(SAME))

    def part_of(ref, p):
        return ref.at[pl.ds(p * (per // PARTS), per // PARTS)]

    def scatter(s, p):
        to = peer(order[s])
        return copy(
            part_of(parcel.at[chunk_of(r, to)], p), part_of(landed.at[s], p),
            send1.at[s], recv1.at[PARTS * s + p], (r, to),
        )

    def scatter_rest(j, p):
        to = owner(r, h * half_n + j)
        return copy(part_of(rest.at[j], p), part_of(landed_rest, p), send_rest.at[j], recv_rest.at[p], (r, to))

    def spare_cos():
        tile = cos.at[pl.ds(4 * TILE, TILE)]
        return copy(tile, tile, send_x.at[0], recv_x.at[0], (partner, c))

    def spare_rows():
        return copy(rows.at[:, tile_at(spare)], rows_x, send_x.at[1], recv_x.at[1], (partner, c))

    for s in range(len(order)):
        scatter(s, 0).start()

    @pl.when(diagonal)
    def _():
        for j in range(half_n):
            k = h * half_n + j
            rest[j] = (part[k] - parcel[k].astype(jnp.float32)).astype(jnp.bfloat16)

    for p in range(PARTS):
        @pl.when(diagonal)
        def _():
            for j in range(half_n):
                @pl.when(me != h * half_n + j)
                def _():
                    scatter_rest(j, p).start()

        if p + 1 < PARTS:
            for s in range(len(order)):
                scatter(s, p + 1).start()

    def generate(base, store, count=LEVELS):
        def strip(s, carry):
            at = pl.multiple_of(s * STRIP, STRIP)
            value = cos[pl.ds(base + at, STRIP), :]
            double = value + value
            before, now = value, jnp.ones_like(value)
            for k in range(count):
                store(k, at, now.astype(jnp.bfloat16))
                before, now = now, double * now - before
            return carry

        return strip

    def generate_pair(t):
        def store(k, at, value):
            cheb[k, t, pl.ds(at, STRIP), :] = value

        loads[2 + 2 * t].wait()
        loads[3 + 2 * t].wait()
        lax.fori_loop(0, 2 * TILE // STRIP, generate(2 * t * TILE, store), 0)

    @pl.when(diagonal)
    def _():
        spare_load.wait()
        spare_cos().start()

    generate_pair(0)

    @pl.when(diagonal)
    def _():
        def store(k, at, value):
            if k >= HALF:
                cheb_x[k - HALF, pl.ds(at, STRIP), :] = value

        lax.fori_loop(0, TILE // STRIP, generate(4 * TILE, store), 0)


    chunk_half = me // half_n
    has_rest = c != 2 * r + chunk_half

    def place(ref, k):
        return ref.at[
            pl.ds(pl.multiple_of(lax.rem(k, 2) * per, per), per),
            pl.ds(pl.multiple_of((k // 2) * width, width), width),
        ]

    def gather(s, cut=lambda ref: ref):
        return copy(cut(mine), cut(place(rows, me)), send2.at[s], recv2.at[me], (r, peer(order[s])))

    def gathered(k):
        return copy(mine, place(rows, k), send2.at[0], recv2.at[k], (r, owner(r, k)))

    def column(e, cut=lambda ref: ref):
        return copy(
            cut(mine), cut(place(cols, lax.rem(me, half_n))), send3.at[e // 2 - 1], recv3.at[lax.rem(me, half_n)],
            (line(e), 2 * r + chunk_half),
        )

    def wanted(to):
        parity = jnp.where(to // 2 < r, chunk_half, 1 - chunk_half)
        return jnp.logical_or(to // 2 == r, lax.rem(to, 2) == parity)

    for p in range(PARTS):
        cut = functools.partial(part_of, p=p)
        span = slice(p * (per // PARTS), (p + 1) * (per // PARTS))
        sum_value = part[me, span]
        for s in range(len(order)):
            scatter(s, p).wait_recv()
            sum_value = sum_value + landed[s, span].astype(jnp.float32)
        part[me, span] = sum_value

        @pl.when(has_rest)
        def _():
            copy(
                part_of(rest.at[0], p), part_of(landed_rest, p), send_rest.at[0], recv_rest.at[p],
                (r, 2 * r + chunk_half),
            ).wait_recv()
            part[me, span] = part[me, span] + landed_rest[span].astype(jnp.float32)

        mine[span] = part[me, span].astype(jnp.bfloat16)
        for e in SAME:
            column(e, cut).start()
        for s in range(len(order)):
            @pl.when(wanted(peer(order[s])))
            def _():
                gather(s, cut).start()
    rows[
        pl.ds(pl.multiple_of(lax.rem(me, 2) * per, per), per),
        pl.ds(pl.multiple_of((me // 2) * width, width), width),
    ] = mine[...]

    generate_pair(1)

    @pl.when(helper)
    def _():
        def store(k, at, value):
            cheb_x[k, pl.ds(at, STRIP), :] = value

        spare_cos().wait_recv()
        lax.fori_loop(0, TILE // STRIP, generate(4 * TILE, store, HALF), 0)

    def relay(j, source):
        return copy(source, place(cols, j), send_r.at[j], recv3.at[j], (partner, c))

    def arrived(j):
        return copy(mine, place(cols, j), send3.at[0], recv3.at[j], (q, owner(q, h * half_n + j)))

    @pl.when(jnp.logical_and(off, relays))
    def _():
        for j in range(half_n):
            arrived(j).wait_recv()
            relay(j, place(cols, j)).start()

    @pl.when(diagonal)
    def _():
        for j in range(half_n):
            k = h * half_n + j

            @pl.when(me != k)
            def _():
                gathered(k).wait_recv()

            relay(j, place(rows, k)).start()

    for k in range(n):
        needed = jnp.where(diagonal, h != k // half_n, side == k // half_n)

        @pl.when(jnp.logical_and(needed, me != k))
        def _():
            gathered(k).wait_recv()

    @pl.when(relayed)
    def _():
        for j in range(half_n):
            arrived(j).wait_recv()

    @pl.when(diagonal)
    def _():
        spare_rows().start()
        size = cols.shape[1]
        cols[...] = rows[:, pl.ds(pl.multiple_of(h * size, size), size)]

    for s in range(len(order)):
        @pl.when(jnp.logical_not(wanted(peer(order[s]))))
        def _():
            gather(s).start()

    weight = jnp.where(diagonal, 1, 2).astype(jnp.float32)
    for t in range(2):
        lhs[t, :, :TILE] = (rows[:, tile_at(first[t])].astype(jnp.float32) * weight).astype(jnp.bfloat16)
        lhs[t, :, TILE:] = (rows[:, tile_at(second[t])].astype(jnp.float32) * 2.0).astype(jnp.bfloat16)
        fj[t] = cols[:, t * TILE : (t + 1) * TILE].astype(jnp.float32)

    matrix_load.wait()
    total[...] = jnp.zeros_like(total)

    def add_moment(acc, prod, k):
        narrow = prod[:, :LANES] + prod[:, LANES:]
        return acc + jnp.sum(narrow, axis=-1, keepdims=True) * matrix[pl.ds(k, 1), :]

    def level_step(step, carry):
        acc = total[...]
        for u in range(UNROLL):
            k = step * UNROLL + u
            prod = None
            for t in range(2):
                image = jnp.dot(lhs[t], cheb[k, t], preferred_element_type=jnp.float32)
                term = image * fj[t]
                prod = term if prod is None else prod + term
            acc = add_moment(acc, prod, k)
        total[...] = acc
        return carry

    lax.fori_loop(0, LEVELS // UNROLL, level_step, 0)

    @pl.when(diagonal)
    def _():
        lhs_x[...] = (rows[:, tile_at(spare)].astype(jnp.float32) * 2.0).astype(jnp.bfloat16)

    @pl.when(helper)
    def _():
        spare_rows().wait_recv()
        lhs_x[...] = (rows_x[...].astype(jnp.float32) * 2.0).astype(jnp.bfloat16)

    @pl.when(jnp.logical_or(diagonal, helper))
    def _():
        base = jnp.where(diagonal, HALF, 0)

        def spare_step(step, carry):
            acc = total[...]
            for u in range(SPARE_UNROLL):
                k = step * SPARE_UNROLL + u
                image = jnp.dot(lhs_x[...], cheb_x[k], preferred_element_type=jnp.float32)
                acc = add_moment(acc, image * fj[h], base + k)
            total[...] = acc
            return carry

        lax.fori_loop(0, HALF // SPARE_UNROLL, spare_step, 0)

    share[...] = total[...].T[:L]

    chips = n_rows // 2
    piece = L // chips
    core, y = lax.rem(r, 2), r // 2

    def block(k):
        return pl.ds(pl.multiple_of(k * piece, piece), piece)

    def across(d):
        return lax.rem(y + d, chips)

    def reduce_line(d, source=core):
        k = across(d)
        return copy(
            share.at[block(k)], line_landed.at[2 * d + source], send4.at[d], recv4.at[2 * d + source],
            (2 * k + 1, c),
        )

    def exchange(s):
        return copy(line_sum, plane_landed.at[c], send5.at[s], recv5.at[s], (r, peer(order[s])))

    def spread_line(d, target, k):
        return copy(
            result, spectra_out.at[block(k)], send6.at[2 * d + target], recv6.at[d], (2 * across(d) + target, c)
        )

    def finish_rows():
        for k in range(n):
            needed = jnp.logical_or(diagonal, side == k // half_n)

            @pl.when(jnp.logical_and(jnp.logical_not(needed), me != k))
            def _():
                gathered(k).wait_recv()

    for d in (2, 3, 1):
        reduce_line(d).start()

    @pl.when(jnp.logical_not(lead))
    def _():
        reduce_line(0, 0).start()

    finish_rows()

    @pl.when(lead)
    def _():
        value = share[block(y)]
        for d, source in ((0, 0), (1, 0), (1, 1), (3, 0), (3, 1), (2, 0), (2, 1)):
            reduce_line(d, source).wait_recv()
            value = value + line_landed[2 * d + source]
        line_sum[...] = value
        for s in range(len(order)):
            exchange(s).start()
        plane_landed[c] = value
        for s in range(len(order)):
            exchange(s).wait_recv()
        value = plane_landed[0]
        for k in range(1, n):
            value = value + plane_landed[k]
        result[...] = value
        for d in (2, 3, 1):
            for target in range(2):
                spread_line(d, target, y).start()
        spread_line(0, 0, y).start()
        spectra_out[block(y)] = value

    for d in (1, 3, 2):
        spread_line(d, 0, lax.rem(y - d + chips, chips)).wait_recv()

    @pl.when(jnp.logical_not(lead))
    def _():
        spread_line(0, 0, y).wait_recv()
        reduce_line(0, 0).wait_send()

    for d in (1, 2, 3):
        reduce_line(d).wait_send()

    @pl.when(lead)
    def _():
        for s in range(len(order)):
            exchange(s).wait_send()
        for d in (1, 2, 3):
            for target in range(2):
                spread_line(d, target, y).wait_send()
        spread_line(0, 0, y).wait_send()

    @pl.when(relays)
    def _():
        for j in range(half_n):
            relay(j, place(cols, j)).wait_send()

    for s in range(len(order)):
        copy(parcel.at[0], landed.at[s], send1.at[s], recv1.at[s], (r, peer(order[s]))).wait_send()
        gather(s).wait_send()
    for e in SAME:
        column(e).wait_send()

    @pl.when(diagonal)
    def _():
        spare_cos().wait_send()
        spare_rows().wait_send()
        for j in range(half_n):
            @pl.when(me != h * half_n + j)
            def _():
                copy(rest.at[j], landed_rest, send_rest.at[j], recv_rest.at[0], (r, c)).wait_send()


def close_kernel(filtered, spectra, filtered_out, spectra_out, sem):
    copies = [
        pltpu.make_async_copy(filtered, filtered_out, sem.at[0]),
        pltpu.make_async_copy(spectra, spectra_out, sem.at[1]),
    ]
    for copy in copies:
        copy.start()
    for copy in copies:
        copy.wait()


def per_device(npix, n_rows, n_cols, inverse_cov, cosines, sky_maps):
    n_z = n_cols // N_X
    n = n_cols
    size, cols_here = inverse_cov.shape
    maps = sky_maps.shape[1]
    sky_t = sky_maps.T
    per, width = maps // 2, 2 * size // n
    piece = L // (n_rows // 2)
    vmem = pl.BlockSpec(memory_space=pltpu.VMEM)
    hbm = pl.BlockSpec(memory_space=pltpu.HBM)
    matrix = jnp.asarray(transform_matrix(npix))
    inputs = (sky_t, inverse_cov, cosines, matrix)
    bf16, f32 = jnp.bfloat16, jnp.float32
    plane = pltpu.SemaphoreType.DMA((n - 1,))
    line = pltpu.SemaphoreType.DMA((n_rows - 1,))
    half = pltpu.SemaphoreType.DMA((n // 2,))
    every = pltpu.SemaphoreType.DMA((n_rows,))
    filtered, spectra = pl.pallas_call(
        functools.partial(qml_kernel, n_rows, n_z, N_X),
        out_shape=(
            jax.ShapeDtypeStruct((maps, size), bf16),
            jax.ShapeDtypeStruct((L, maps), f32),
        ),
        in_specs=[hbm] * len(inputs),
        out_specs=(vmem, vmem),
        scratch_shapes=[
            pltpu.VMEM(sky_t.shape, bf16),
            pltpu.VMEM(inverse_cov.shape, bf16),
            pltpu.VMEM((5 * TILE, TILE), f32),
            pltpu.VMEM(matrix.shape, f32),
            pltpu.VMEM((LEVELS, 2, 2 * TILE, TILE), bf16),
            pltpu.VMEM((HALF, TILE, TILE), bf16),
            pltpu.VMEM((n, per, width), f32),
            pltpu.VMEM((n, per, width), bf16),
            pltpu.VMEM((n - 1, per, width), bf16),
            pltpu.VMEM((n // 2, per, width), bf16),
            pltpu.VMEM((per, width), bf16),
            pltpu.VMEM((per, width), bf16),
            pltpu.VMEM((maps, cols_here), bf16),
            pltpu.VMEM((2, maps, 2 * TILE), bf16),
            pltpu.VMEM((maps, TILE), bf16),
            pltpu.VMEM((maps, TILE), bf16),
            pltpu.VMEM((2, maps, TILE), f32),
            pltpu.VMEM((maps, LANES), f32),
            pltpu.VMEM((L, maps), f32),
            pltpu.VMEM((n_rows, piece, maps), f32),
            pltpu.VMEM((piece, maps), f32),
            pltpu.VMEM((n, piece, maps), f32),
            pltpu.VMEM((piece, maps), f32),
            pltpu.SemaphoreType.DMA((8,)),
            plane, pltpu.SemaphoreType.DMA((PARTS * (n - 1),)), half, pltpu.SemaphoreType.DMA((PARTS,)),
            plane, pltpu.SemaphoreType.DMA((n,)),
            line, half, line, every, plane, plane, every, line,
            pltpu.SemaphoreType.DMA((2,)), pltpu.SemaphoreType.DMA((2,)), half,
        ],
        compiler_params=pltpu.CompilerParams(
            collective_id=1, has_side_effects=True, vmem_limit_bytes=50 * 2**20
        ),
        name="qml",
    )(*[pltpu.with_memory_space_constraint(value, pltpu.HBM) for value in inputs])
    filtered, spectra = pl.pallas_call(
        close_kernel,
        out_shape=(pltpu.HBM(filtered.shape, bf16), pltpu.HBM(spectra.shape, f32)),
        in_specs=[vmem, vmem],
        out_specs=(hbm, hbm),
        scratch_shapes=[pltpu.SemaphoreType.DMA((2,))],
        compiler_params=pltpu.CompilerParams(vmem_limit_bytes=2**20),
        name="close",
    )(filtered, spectra)
    return filtered.T, spectra


def solution(mesh):
    in_specs = (P("prow", "pcol"), P("prow", "pcol"), P("pcol", None))
    out_specs = (P("prow", None), P())
    n_rows, n_cols = mesh.shape["prow"], mesh.shape["pcol"]

    def whole(inverse_cov, cosines, sky_maps):
        npix = cosines.shape[0]
        step = jax.shard_map(
            functools.partial(per_device, npix, n_rows, n_cols),
            mesh=mesh, in_specs=in_specs, out_specs=out_specs, check_vma=False,
        )
        return step(inverse_cov, cosines, sky_maps)

    return whole
```

```python
import functools
import math

import jax
import jax.numpy as jnp
import numpy as np
from jax import lax
from jax.experimental import pallas as pl
from jax.experimental.pallas import tpu as pltpu
from jax.sharding import PartitionSpec as P

L = 64
LMIN = 2
TOP = LMIN + L - 1
LEVELS = TOP + 1
UNROLL = 22
HALF = LEVELS // 2
SPARE_UNROLL = 33
TILE = 256
STRIP = 32
N_X = 4
PARTS = 2
LANES = 128
MESH = pl.DeviceIdType.MESH


def transform_matrix(npix):
    a = [math.comb(2 * k, k) / 4.0**k for k in range(TOP + 1)]
    out = np.zeros((-(-LEVELS // 8) * 8, LANES))
    for l in range(LMIN, TOP + 1):
        for k in range(l + 1):
            out[abs(l - 2 * k), l - LMIN] += a[k] * a[l - k] * (2 * l + 1) / npix
    return out.astype(np.float32)


def rank_order(rows, cols):
    spots = [(dz, dx) for dz in range(rows) for dx in range(cols) if dz or dx]
    reach = lambda d, n: min(d, n - d)
    return sorted(spots, key=lambda s: -(reach(s[0], rows) + reach(s[1], cols)))


LINE = [4, 5, 3, 2, 6, 1, 7]
SAME = [4, 2, 6]


def qml_kernel(
    n_rows, n_z, n_x,
    sky_hbm, cov_hbm, cos_hbm, matrix_hbm,
    rows, spectra_out,
    sky, cov, cos, matrix, cheb, cheb_x, part, parcel, landed, rest, landed_rest, mine, cols,
    lhs, lhs_x, rows_x, fj, total, share, line_landed, line_sum, plane_landed, result,
    load_sem, send1, recv1, send_rest, recv_rest, send2, recv2, send3, recv3,
    send4, recv4, send5, recv5, send6, recv6, send_x, recv_x, send_r,
):
    r = lax.axis_index("prow")
    c = lax.axis_index("pcol")
    n = n_z * n_x
    z, x = c // n_x, lax.rem(c, n_x)
    q, h = c // 2, lax.rem(c, 2)
    half_n = n // 2
    maps = sky.shape[0]
    per, width = parcel.shape[1], parcel.shape[2]
    order = rank_order(n_z, n_x)
    diagonal = r == q
    off = r != q
    partner = r + 1 - 2 * lax.rem(r, 2)
    helper = partner == q
    lead = lax.rem(r, 2) == 1
    relays = jnp.logical_or(diagonal, jnp.logical_and(r // 2 != q // 2, lead))
    relayed = jnp.logical_not(relays)
    side = jnp.where(r > q, h, 1 - h)
    barrier = pltpu.get_barrier_semaphore()

    def peer(spot):
        return lax.rem(z + spot[0], n_z) * n_x + lax.rem(x + spot[1], n_x)

    def line(e):
        return lax.rem(r + e, n_rows)

    def turn(row):
        return n_x // 2 * lax.rem(row, 2) + n_x - 1

    def chunk_of(row, col):
        return lax.rem(lax.rem(col, n_x) - turn(row) + 2 * n_x, n_x) * n_z + col // n_x

    def owner(row, k):
        return (k % n_z if isinstance(k, int) else lax.rem(k, n_z)) * n_x + lax.rem(k // n_z + turn(row), n_x)

    me = chunk_of(r, c)

    def signal(device):
        pl.semaphore_signal(barrier, inc=1, device_id=device, device_id_type=MESH)

    def copy(src, dst, send, recv, device):
        return pltpu.make_async_remote_copy(
            src_ref=src, dst_ref=dst, send_sem=send, recv_sem=recv,
            device_id=device, device_id_type=MESH,
        )

    first = [jnp.where(diagonal, 2 * h, 2 * side), jnp.where(diagonal, 1 + 2 * h, 2 * side)]
    second = [jnp.where(diagonal, 2 * h + 1, 2 * side + 1), jnp.where(diagonal, 2 - 2 * h, 2 * side + 1)]
    spare = 2 - h

    def tile_at(index):
        return pl.ds(pl.multiple_of(index * TILE, TILE), TILE)

    loads = [
        pltpu.make_async_copy(sky_hbm, sky, load_sem.at[0]),
        pltpu.make_async_copy(cov_hbm, cov, load_sem.at[1]),
    ]
    for t in range(2):
        for s, row in enumerate((first[t], second[t])):
            loads.append(
                pltpu.make_async_copy(
                    cos_hbm.at[tile_at(row), pl.ds(t * TILE, TILE)],
                    cos.at[pl.ds((2 * t + s) * TILE, TILE)],
                    load_sem.at[2 + 2 * t + s],
                )
            )
    matrix_load = pltpu.make_async_copy(matrix_hbm, matrix, load_sem.at[7])
    spare_load = pltpu.make_async_copy(
        cos_hbm.at[tile_at(spare), tile_at(h)], cos.at[pl.ds(4 * TILE, TILE)], load_sem.at[6]
    )
    for load in loads[:2]:
        load.start()

    for spot in order:
        signal((r, peer(spot)))
    for e in LINE:
        signal((line(e), c))

    @pl.when(jnp.logical_and(off, relays))
    def _():
        for j in range(half_n):
            signal((q, owner(q, h * half_n + j)))

    loads[0].wait()
    loads[1].wait()
    for load in loads[2:]:
        load.start()
    matrix_load.start()

    @pl.when(diagonal)
    def _():
        spare_load.start()

    wide = 2 * width
    for g in range(cov.shape[0] // wide):
        value = lax.dot_general(
            sky[...], cov[g * wide : (g + 1) * wide, :], (((1,), (1,)), ((), ())),
            preferred_element_type=jnp.float32,
        )
        for a in range(2):
            for b in range(maps // per):
                k = (2 * g + a) * (maps // per) + b
                piece = value[b * per : (b + 1) * per, a * width : (a + 1) * width]
                part[k] = piece
                parcel[k] = piece.astype(jnp.bfloat16)

    pl.semaphore_wait(barrier, len(order) + len(LINE) + len(SAME))

    def part_of(ref, p):
        return ref.at[pl.ds(p * (per // PARTS), per // PARTS)]

    def scatter(s, p):
        to = peer(order[s])
        return copy(
            part_of(parcel.at[chunk_of(r, to)], p), part_of(landed.at[s], p),
            send1.at[s], recv1.at[PARTS * s + p], (r, to),
        )

    def scatter_rest(j, p):
        to = owner(r, h * half_n + j)
        return copy(part_of(rest.at[j], p), part_of(landed_rest, p), send_rest.at[j], recv_rest.at[p], (r, to))

    def spare_cos():
        tile = cos.at[pl.ds(4 * TILE, TILE)]
        return copy(tile, tile, send_x.at[0], recv_x.at[0], (partner, c))

    def spare_rows():
        return copy(rows.at[:, tile_at(spare)], rows_x, send_x.at[1], recv_x.at[1], (partner, c))

    for s in range(len(order)):
        scatter(s, 0).start()

    @pl.when(diagonal)
    def _():
        for j in range(half_n):
            k = h * half_n + j
            rest[j] = (part[k] - parcel[k].astype(jnp.float32)).astype(jnp.bfloat16)

    for p in range(PARTS):
        @pl.when(diagonal)
        def _():
            for j in range(half_n):
                @pl.when(me != h * half_n + j)
                def _():
                    scatter_rest(j, p).start()

        if p + 1 < PARTS:
            for s in range(len(order)):
                scatter(s, p + 1).start()

    def generate(base, store, count=LEVELS):
        def strip(s, carry):
            at = pl.multiple_of(s * STRIP, STRIP)
            value = cos[pl.ds(base + at, STRIP), :]
            double = value + value
            before, now = value, jnp.ones_like(value)
            for k in range(count):
                store(k, at, now.astype(jnp.bfloat16))
                before, now = now, double * now - before
            return carry

        return strip

    def generate_pair(t):
        def store(k, at, value):
            cheb[k, t, pl.ds(at, STRIP), :] = value

        loads[2 + 2 * t].wait()
        loads[3 + 2 * t].wait()
        lax.fori_loop(0, 2 * TILE // STRIP, generate(2 * t * TILE, store), 0)

    @pl.when(diagonal)
    def _():
        spare_load.wait()
        spare_cos().start()

    generate_pair(0)

    @pl.when(diagonal)
    def _():
        def store(k, at, value):
            if k >= HALF:
                cheb_x[k - HALF, pl.ds(at, STRIP), :] = value

        lax.fori_loop(0, TILE // STRIP, generate(4 * TILE, store), 0)


    chunk_half = me // half_n
    has_rest = c != 2 * r + chunk_half

    def place(ref, k):
        return ref.at[
            pl.ds(pl.multiple_of(lax.rem(k, 2) * per, per), per),
            pl.ds(pl.multiple_of((k // 2) * width, width), width),
        ]

    def gather(s, cut=lambda ref: ref):
        return copy(cut(mine), cut(place(rows, me)), send2.at[s], recv2.at[me], (r, peer(order[s])))

    def gathered(k):
        return copy(mine, place(rows, k), send2.at[0], recv2.at[k], (r, owner(r, k)))

    def column(e, cut=lambda ref: ref):
        return copy(
            cut(mine), cut(place(cols, lax.rem(me, half_n))), send3.at[e // 2 - 1], recv3.at[lax.rem(me, half_n)],
            (line(e) // 2 * 2 + 1, 2 * r + chunk_half),
        )

    def wanted(to):
        parity = jnp.where(to // 2 < r, chunk_half, 1 - chunk_half)
        return jnp.logical_or(to // 2 == r, lax.rem(to, 2) == parity)

    for p in range(PARTS):
        cut = functools.partial(part_of, p=p)
        span = slice(p * (per // PARTS), (p + 1) * (per // PARTS))
        sum_value = part[me, span]
        for s in range(len(order)):
            scatter(s, p).wait_recv()
            sum_value = sum_value + landed[s, span].astype(jnp.float32)
        part[me, span] = sum_value

        @pl.when(has_rest)
        def _():
            copy(
                part_of(rest.at[0], p), part_of(landed_rest, p), send_rest.at[0], recv_rest.at[p],
                (r, 2 * r + chunk_half),
            ).wait_recv()
            part[me, span] = part[me, span] + landed_rest[span].astype(jnp.float32)

        mine[span] = part[me, span].astype(jnp.bfloat16)
        for e in SAME:
            column(e, cut).start()
        for s in range(len(order)):
            @pl.when(wanted(peer(order[s])))
            def _():
                gather(s, cut).start()
    rows[
        pl.ds(pl.multiple_of(lax.rem(me, 2) * per, per), per),
        pl.ds(pl.multiple_of((me // 2) * width, width), width),
    ] = mine[...]

    generate_pair(1)

    @pl.when(helper)
    def _():
        def store(k, at, value):
            cheb_x[k, pl.ds(at, STRIP), :] = value

        spare_cos().wait_recv()
        lax.fori_loop(0, TILE // STRIP, generate(4 * TILE, store, HALF), 0)

    def relay(j, source):
        return copy(source, place(cols, j), send_r.at[j], recv3.at[j], (partner, c))

    def arrived(j):
        return copy(mine, place(cols, j), send3.at[0], recv3.at[j], (q, owner(q, h * half_n + j)))

    @pl.when(jnp.logical_and(off, relays))
    def _():
        for j in range(half_n):
            arrived(j).wait_recv()
            relay(j, place(cols, j)).start()
        for t in range(2):
            fj[t] = cols[:, t * TILE : (t + 1) * TILE].astype(jnp.float32)

    @pl.when(diagonal)
    def _():
        for j in range(half_n):
            k = h * half_n + j

            @pl.when(me != k)
            def _():
                gathered(k).wait_recv()

            relay(j, place(rows, k)).start()
        for t in range(2):
            fj[t] = rows[:, tile_at(2 * h + t)].astype(jnp.float32)

    for k in range(n):
        needed = jnp.where(diagonal, h != k // half_n, side == k // half_n)

        @pl.when(jnp.logical_and(needed, me != k))
        def _():
            gathered(k).wait_recv()

    @pl.when(diagonal)
    def _():
        spare_rows().start()

    for s in range(len(order)):
        @pl.when(jnp.logical_not(wanted(peer(order[s]))))
        def _():
            gather(s).start()

    weight = jnp.where(diagonal, 1, 2).astype(jnp.float32)
    for t in range(2):
        lhs[t, :, :TILE] = (rows[:, tile_at(first[t])].astype(jnp.float32) * weight).astype(jnp.bfloat16)
        lhs[t, :, TILE:] = (rows[:, tile_at(second[t])].astype(jnp.float32) * 2.0).astype(jnp.bfloat16)

    @pl.when(relayed)
    def _():
        for j in range(half_n):
            arrived(j).wait_recv()
        for t in range(2):
            fj[t] = cols[:, t * TILE : (t + 1) * TILE].astype(jnp.float32)

    matrix_load.wait()
    total[...] = jnp.zeros_like(total)

    def add_moment(acc, prod, k):
        narrow = prod[:, :LANES] + prod[:, LANES:]
        return acc + jnp.sum(narrow, axis=-1, keepdims=True) * matrix[pl.ds(k, 1), :]

    def level_step(step, carry):
        acc = total[...]
        for u in range(UNROLL):
            k = step * UNROLL + u
            prod = None
            for t in range(2):
                image = jnp.dot(lhs[t], cheb[k, t], preferred_element_type=jnp.float32)
                term = image * fj[t]
                prod = term if prod is None else prod + term
            acc = add_moment(acc, prod, k)
        total[...] = acc
        return carry

    lax.fori_loop(0, LEVELS // UNROLL, level_step, 0)

    @pl.when(diagonal)
    def _():
        lhs_x[...] = (rows[:, tile_at(spare)].astype(jnp.float32) * 2.0).astype(jnp.bfloat16)

    @pl.when(helper)
    def _():
        spare_rows().wait_recv()
        lhs_x[...] = (rows_x[...].astype(jnp.float32) * 2.0).astype(jnp.bfloat16)

    @pl.when(jnp.logical_or(diagonal, helper))
    def _():
        base = jnp.where(diagonal, HALF, 0)

        def spare_step(step, carry):
            acc = total[...]
            for u in range(SPARE_UNROLL):
                k = step * SPARE_UNROLL + u
                image = jnp.dot(lhs_x[...], cheb_x[k], preferred_element_type=jnp.float32)
                acc = add_moment(acc, image * fj[h], base + k)
            total[...] = acc
            return carry

        lax.fori_loop(0, HALF // SPARE_UNROLL, spare_step, 0)

    share[...] = total[...].T[:L]

    chips = n_rows // 2
    piece = L // chips
    core, y = lax.rem(r, 2), r // 2

    def block(k):
        return pl.ds(pl.multiple_of(k * piece, piece), piece)

    def across(d):
        return lax.rem(y + d, chips)

    def reduce_line(d, source=core):
        k = across(d)
        return copy(
            share.at[block(k)], line_landed.at[2 * d + source], send4.at[d], recv4.at[2 * d + source],
            (2 * k + 1, c),
        )

    def exchange(s):
        return copy(line_sum, plane_landed.at[c], send5.at[s], recv5.at[s], (r, peer(order[s])))

    def spread_line(d, target, k):
        return copy(
            result, spectra_out.at[block(k)], send6.at[2 * d + target], recv6.at[d], (2 * across(d) + target, c)
        )

    def finish_rows():
        for k in range(n):
            needed = jnp.logical_or(diagonal, side == k // half_n)

            @pl.when(jnp.logical_and(jnp.logical_not(needed), me != k))
            def _():
                gathered(k).wait_recv()

    for d in (2, 3, 1):
        reduce_line(d).start()

    @pl.when(jnp.logical_not(lead))
    def _():
        reduce_line(0, 0).start()

    finish_rows()

    @pl.when(lead)
    def _():
        value = share[block(y)]
        for d, source in ((0, 0), (1, 0), (1, 1), (3, 0), (3, 1), (2, 0), (2, 1)):
            reduce_line(d, source).wait_recv()
            value = value + line_landed[2 * d + source]
        line_sum[...] = value
        for s in range(len(order)):
            exchange(s).start()
        plane_landed[c] = value
        for s in range(len(order)):
            exchange(s).wait_recv()
        value = plane_landed[0]
        for k in range(1, n):
            value = value + plane_landed[k]
        result[...] = value
        for d in (2, 3, 1):
            for target in range(2):
                spread_line(d, target, y).start()
        spread_line(0, 0, y).start()
        spectra_out[block(y)] = value

    for d in (1, 3, 2):
        spread_line(d, 0, lax.rem(y - d + chips, chips)).wait_recv()

    @pl.when(jnp.logical_not(lead))
    def _():
        spread_line(0, 0, y).wait_recv()
        reduce_line(0, 0).wait_send()

    for d in (1, 2, 3):
        reduce_line(d).wait_send()

    @pl.when(lead)
    def _():
        for s in range(len(order)):
            exchange(s).wait_send()
        for d in (1, 2, 3):
            for target in range(2):
                spread_line(d, target, y).wait_send()
        spread_line(0, 0, y).wait_send()

    @pl.when(relays)
    def _():
        for j in range(half_n):
            relay(j, place(cols, j)).wait_send()

    for s in range(len(order)):
        copy(parcel.at[0], landed.at[s], send1.at[s], recv1.at[s], (r, peer(order[s]))).wait_send()
        gather(s).wait_send()
    for e in SAME:
        column(e).wait_send()

    @pl.when(diagonal)
    def _():
        spare_cos().wait_send()
        spare_rows().wait_send()
        for j in range(half_n):
            @pl.when(me != h * half_n + j)
            def _():
                copy(rest.at[j], landed_rest, send_rest.at[j], recv_rest.at[0], (r, c)).wait_send()


def close_kernel(filtered, spectra, filtered_out, spectra_out, sem):
    copies = [
        pltpu.make_async_copy(filtered, filtered_out, sem.at[0]),
        pltpu.make_async_copy(spectra, spectra_out, sem.at[1]),
    ]
    for copy in copies:
        copy.start()
    for copy in copies:
        copy.wait()


def per_device(npix, n_rows, n_cols, inverse_cov, cosines, sky_maps):
    n_z = n_cols // N_X
    n = n_cols
    size, cols_here = inverse_cov.shape
    maps = sky_maps.shape[1]
    sky_t = sky_maps.T
    per, width = maps // 2, 2 * size // n
    piece = L // (n_rows // 2)
    vmem = pl.BlockSpec(memory_space=pltpu.VMEM)
    hbm = pl.BlockSpec(memory_space=pltpu.HBM)
    matrix = jnp.asarray(transform_matrix(npix))
    inputs = (sky_t, inverse_cov, cosines, matrix)
    bf16, f32 = jnp.bfloat16, jnp.float32
    plane = pltpu.SemaphoreType.DMA((n - 1,))
    line = pltpu.SemaphoreType.DMA((n_rows - 1,))
    half = pltpu.SemaphoreType.DMA((n // 2,))
    every = pltpu.SemaphoreType.DMA((n_rows,))
    filtered, spectra = pl.pallas_call(
        functools.partial(qml_kernel, n_rows, n_z, N_X),
        out_shape=(
            jax.ShapeDtypeStruct((maps, size), bf16),
            jax.ShapeDtypeStruct((L, maps), f32),
        ),
        in_specs=[hbm] * len(inputs),
        out_specs=(vmem, vmem),
        scratch_shapes=[
            pltpu.VMEM(sky_t.shape, bf16),
            pltpu.VMEM(inverse_cov.shape, bf16),
            pltpu.VMEM((5 * TILE, TILE), f32),
            pltpu.VMEM(matrix.shape, f32),
            pltpu.VMEM((LEVELS, 2, 2 * TILE, TILE), bf16),
            pltpu.VMEM((HALF, TILE, TILE), bf16),
            pltpu.VMEM((n, per, width), f32),
            pltpu.VMEM((n, per, width), bf16),
            pltpu.VMEM((n - 1, per, width), bf16),
            pltpu.VMEM((n // 2, per, width), bf16),
            pltpu.VMEM((per, width), bf16),
            pltpu.VMEM((per, width), bf16),
            pltpu.VMEM((maps, cols_here), bf16),
            pltpu.VMEM((2, maps, 2 * TILE), bf16),
            pltpu.VMEM((maps, TILE), bf16),
            pltpu.VMEM((maps, TILE), bf16),
            pltpu.VMEM((2, maps, TILE), f32),
            pltpu.VMEM((maps, LANES), f32),
            pltpu.VMEM((L, maps), f32),
            pltpu.VMEM((n_rows, piece, maps), f32),
            pltpu.VMEM((piece, maps), f32),
            pltpu.VMEM((n, piece, maps), f32),
            pltpu.VMEM((piece, maps), f32),
            pltpu.SemaphoreType.DMA((8,)),
            plane, pltpu.SemaphoreType.DMA((PARTS * (n - 1),)), half, pltpu.SemaphoreType.DMA((PARTS,)),
            plane, pltpu.SemaphoreType.DMA((n,)),
            line, half, line, every, plane, plane, every, line,
            pltpu.SemaphoreType.DMA((2,)), pltpu.SemaphoreType.DMA((2,)), half,
        ],
        compiler_params=pltpu.CompilerParams(
            collective_id=1, has_side_effects=True, vmem_limit_bytes=50 * 2**20
        ),
        name="qml",
    )(*[pltpu.with_memory_space_constraint(value, pltpu.HBM) for value in inputs])
    filtered, spectra = pl.pallas_call(
        close_kernel,
        out_shape=(pltpu.HBM(filtered.shape, bf16), pltpu.HBM(spectra.shape, f32)),
        in_specs=[vmem, vmem],
        out_specs=(hbm, hbm),
        scratch_shapes=[pltpu.SemaphoreType.DMA((2,))],
        compiler_params=pltpu.CompilerParams(vmem_limit_bytes=2**20),
        name="close",
    )(filtered, spectra)
    return filtered.T, spectra


def solution(mesh):
    in_specs = (P("prow", "pcol"), P("prow", "pcol"), P("pcol", None))
    out_specs = (P("prow", None), P())
    n_rows, n_cols = mesh.shape["prow"], mesh.shape["pcol"]

    def whole(inverse_cov, cosines, sky_maps):
        npix = cosines.shape[0]
        step = jax.shard_map(
            functools.partial(per_device, npix, n_rows, n_cols),
            mesh=mesh, in_specs=in_specs, out_specs=out_specs, check_vma=False,
        )
        return step(inverse_cov, cosines, sky_maps)

    return whole
```

```python
import functools
import math

import jax
import jax.numpy as jnp
import numpy as np
from jax import lax
from jax.experimental import pallas as pl
from jax.experimental.pallas import tpu as pltpu
from jax.sharding import PartitionSpec as P

L = 64
LMIN = 2
TOP = LMIN + L - 1
LEVELS = TOP + 1
UNROLL = 22
HALF = LEVELS // 2
SPARE_UNROLL = 33
TILE = 256
STRIP = 32
N_X = 4
PARTS = 2
LANES = 128
MESH = pl.DeviceIdType.MESH


def transform_matrix(npix):
    a = [math.comb(2 * k, k) / 4.0**k for k in range(TOP + 1)]
    out = np.zeros((-(-LEVELS // 8) * 8, LANES))
    for l in range(LMIN, TOP + 1):
        for k in range(l + 1):
            out[abs(l - 2 * k), l - LMIN] += a[k] * a[l - k] * (2 * l + 1) / npix
    return out.astype(np.float32)


def rank_order(rows, cols):
    spots = [
        (2, 2), (1, 1), (3, 3), (1, 3), (3, 1), (2, 1), (1, 2), (2, 3), (3, 2),
        (0, 1), (1, 0), (0, 3), (3, 0), (0, 2), (2, 0),
    ]
    assert (rows, cols) == (4, 4)
    return spots


LINE = [4, 5, 3, 2, 6, 1, 7]
SAME = [4, 2, 6]


def qml_kernel(
    n_rows, n_z, n_x,
    sky_hbm, cov_hbm, cos_hbm, matrix_hbm,
    rows, spectra_out,
    sky, cov, cos, matrix, cheb, cheb_x, part, parcel, landed, rest, landed_rest, mine, cols,
    lhs, lhs_x, rows_x, fj, total, share, line_landed, line_sum, plane_landed, result,
    load_sem, send1, recv1, send_rest, recv_rest, send2, recv2, send3, recv3,
    send4, recv4, send5, recv5, send6, recv6, send_x, recv_x, send_r,
):
    r = lax.axis_index("prow")
    c = lax.axis_index("pcol")
    n = n_z * n_x
    z, x = c // n_x, lax.rem(c, n_x)
    q, h = c // 2, lax.rem(c, 2)
    half_n = n // 2
    maps = sky.shape[0]
    per, width = parcel.shape[1], parcel.shape[2]
    order = rank_order(n_z, n_x)
    diagonal = r == q
    off = r != q
    partner = r + 1 - 2 * lax.rem(r, 2)
    helper = partner == q
    lead = lax.rem(r, 2) == 1
    relays = jnp.logical_or(diagonal, jnp.logical_and(r // 2 != q // 2, lead))
    relayed = jnp.logical_not(relays)
    side = jnp.where(r > q, h, 1 - h)
    barrier = pltpu.get_barrier_semaphore()

    def peer(spot):
        return lax.rem(z + spot[0], n_z) * n_x + lax.rem(x + spot[1], n_x)

    def line(e):
        return lax.rem(r + e, n_rows)

    def turn(row):
        return n_x // 2 * lax.rem(row, 2) + n_x - 1

    def chunk_of(row, col):
        return lax.rem(lax.rem(col, n_x) - turn(row) + 2 * n_x, n_x) * n_z + col // n_x

    def owner(row, k):
        return (k % n_z if isinstance(k, int) else lax.rem(k, n_z)) * n_x + lax.rem(k // n_z + turn(row), n_x)

    me = chunk_of(r, c)

    def signal(device):
        pl.semaphore_signal(barrier, inc=1, device_id=device, device_id_type=MESH)

    def copy(src, dst, send, recv, device):
        return pltpu.make_async_remote_copy(
            src_ref=src, dst_ref=dst, send_sem=send, recv_sem=recv,
            device_id=device, device_id_type=MESH,
        )

    first = [jnp.where(diagonal, 2 * h, 2 * side), jnp.where(diagonal, 1 + 2 * h, 2 * side)]
    second = [jnp.where(diagonal, 2 * h + 1, 2 * side + 1), jnp.where(diagonal, 2 - 2 * h, 2 * side + 1)]
    spare = 2 - h

    def tile_at(index):
        return pl.ds(pl.multiple_of(index * TILE, TILE), TILE)

    loads = [
        pltpu.make_async_copy(sky_hbm, sky, load_sem.at[0]),
        pltpu.make_async_copy(cov_hbm, cov, load_sem.at[1]),
    ]
    for t in range(2):
        for s, row in enumerate((first[t], second[t])):
            loads.append(
                pltpu.make_async_copy(
                    cos_hbm.at[tile_at(row), pl.ds(t * TILE, TILE)],
                    cos.at[pl.ds((2 * t + s) * TILE, TILE)],
                    load_sem.at[2 + 2 * t + s],
                )
            )
    matrix_load = pltpu.make_async_copy(matrix_hbm, matrix, load_sem.at[7])
    spare_load = pltpu.make_async_copy(
        cos_hbm.at[tile_at(spare), tile_at(h)], cos.at[pl.ds(4 * TILE, TILE)], load_sem.at[6]
    )
    for load in loads[:2]:
        load.start()

    for spot in order:
        signal((r, peer(spot)))
    for e in LINE:
        signal((line(e), c))

    @pl.when(jnp.logical_and(off, relays))
    def _():
        for j in range(half_n):
            signal((q, owner(q, h * half_n + j)))

    loads[0].wait()
    loads[1].wait()
    for load in loads[2:]:
        load.start()
    matrix_load.start()

    @pl.when(diagonal)
    def _():
        spare_load.start()

    wide = 2 * width
    for g in range(cov.shape[0] // wide):
        value = lax.dot_general(
            sky[...], cov[g * wide : (g + 1) * wide, :], (((1,), (1,)), ((), ())),
            preferred_element_type=jnp.float32,
        )
        for a in range(2):
            for b in range(maps // per):
                k = (2 * g + a) * (maps // per) + b
                piece = value[b * per : (b + 1) * per, a * width : (a + 1) * width]
                part[k] = piece
                parcel[k] = piece.astype(jnp.bfloat16)

    pl.semaphore_wait(barrier, len(order) + len(LINE) + len(SAME))

    def part_of(ref, p):
        return ref.at[pl.ds(p * (per // PARTS), per // PARTS)]

    def scatter(s, p):
        to = peer(order[s])
        return copy(
            part_of(parcel.at[chunk_of(r, to)], p), part_of(landed.at[s], p),
            send1.at[s], recv1.at[PARTS * s + p], (r, to),
        )

    def scatter_rest(j, p):
        to = owner(r, h * half_n + j)
        return copy(part_of(rest.at[j], p), part_of(landed_rest, p), send_rest.at[j], recv_rest.at[p], (r, to))

    def spare_cos():
        tile = cos.at[pl.ds(4 * TILE, TILE)]
        return copy(tile, tile, send_x.at[0], recv_x.at[0], (partner, c))

    def spare_rows():
        return copy(rows.at[:, tile_at(spare)], rows_x, send_x.at[1], recv_x.at[1], (partner, c))

    for s in range(len(order)):
        scatter(s, 0).start()

    @pl.when(diagonal)
    def _():
        for j in range(half_n):
            k = h * half_n + j
            rest[j] = (part[k] - parcel[k].astype(jnp.float32)).astype(jnp.bfloat16)

    for p in range(PARTS):
        @pl.when(diagonal)
        def _():
            for j in range(half_n):
                @pl.when(me != h * half_n + j)
                def _():
                    scatter_rest(j, p).start()

        if p + 1 < PARTS:
            for s in range(len(order)):
                scatter(s, p + 1).start()

    def generate(base, store, count=LEVELS):
        def strip(s, carry):
            at = pl.multiple_of(s * STRIP, STRIP)
            value = cos[pl.ds(base + at, STRIP), :]
            double = value + value
            before, now = value, jnp.ones_like(value)
            for k in range(count):
                store(k, at, now.astype(jnp.bfloat16))
                before, now = now, double * now - before
            return carry

        return strip

    def generate_pair(t):
        def store(k, at, value):
            cheb[k, t, pl.ds(at, STRIP), :] = value

        loads[2 + 2 * t].wait()
        loads[3 + 2 * t].wait()
        lax.fori_loop(0, 2 * TILE // STRIP, generate(2 * t * TILE, store), 0)

    @pl.when(diagonal)
    def _():
        spare_load.wait()
        spare_cos().start()

    generate_pair(0)

    @pl.when(diagonal)
    def _():
        def store(k, at, value):
            if k >= HALF:
                cheb_x[k - HALF, pl.ds(at, STRIP), :] = value

        lax.fori_loop(0, TILE // STRIP, generate(4 * TILE, store), 0)


    chunk_half = me // half_n
    has_rest = c != 2 * r + chunk_half

    def place(ref, k):
        return ref.at[
            pl.ds(pl.multiple_of(lax.rem(k, 2) * per, per), per),
            pl.ds(pl.multiple_of((k // 2) * width, width), width),
        ]

    def gather(s, cut=lambda ref: ref):
        return copy(cut(mine), cut(place(rows, me)), send2.at[s], recv2.at[me], (r, peer(order[s])))

    def gathered(k):
        return copy(mine, place(rows, k), send2.at[0], recv2.at[k], (r, owner(r, k)))

    def column(e, cut=lambda ref: ref):
        return copy(
            cut(mine), cut(place(cols, lax.rem(me, half_n))), send3.at[e // 2 - 1], recv3.at[lax.rem(me, half_n)],
            (line(e) // 2 * 2 + 1, 2 * r + chunk_half),
        )

    def wanted(to):
        parity = jnp.where(to // 2 < r, chunk_half, 1 - chunk_half)
        return jnp.logical_or(to // 2 == r, lax.rem(to, 2) == parity)

    for p in range(PARTS):
        cut = functools.partial(part_of, p=p)
        span = slice(p * (per // PARTS), (p + 1) * (per // PARTS))
        sum_value = part[me, span]
        for s in range(len(order)):
            scatter(s, p).wait_recv()
            sum_value = sum_value + landed[s, span].astype(jnp.float32)
        part[me, span] = sum_value

        @pl.when(has_rest)
        def _():
            copy(
                part_of(rest.at[0], p), part_of(landed_rest, p), send_rest.at[0], recv_rest.at[p],
                (r, 2 * r + chunk_half),
            ).wait_recv()
            part[me, span] = part[me, span] + landed_rest[span].astype(jnp.float32)

        mine[span] = part[me, span].astype(jnp.bfloat16)
        for e in SAME:
            column(e, cut).start()
        for s in range(len(order)):
            @pl.when(wanted(peer(order[s])))
            def _():
                gather(s, cut).start()
    rows[
        pl.ds(pl.multiple_of(lax.rem(me, 2) * per, per), per),
        pl.ds(pl.multiple_of((me // 2) * width, width), width),
    ] = mine[...]

    generate_pair(1)

    @pl.when(helper)
    def _():
        def store(k, at, value):
            cheb_x[k, pl.ds(at, STRIP), :] = value

        spare_cos().wait_recv()
        lax.fori_loop(0, TILE // STRIP, generate(4 * TILE, store, HALF), 0)

    def relay(j, source):
        return copy(source, place(cols, j), send_r.at[j], recv3.at[j], (partner, c))

    def arrived(j):
        return copy(mine, place(cols, j), send3.at[0], recv3.at[j], (q, owner(q, h * half_n + j)))

    @pl.when(jnp.logical_and(off, relays))
    def _():
        for j in range(half_n):
            arrived(j).wait_recv()
            relay(j, place(cols, j)).start()
        for t in range(2):
            fj[t] = cols[:, t * TILE : (t + 1) * TILE].astype(jnp.float32)

    @pl.when(diagonal)
    def _():
        for j in range(half_n):
            k = h * half_n + j

            @pl.when(me != k)
            def _():
                gathered(k).wait_recv()

            relay(j, place(rows, k)).start()
        for t in range(2):
            fj[t] = rows[:, tile_at(2 * h + t)].astype(jnp.float32)

    for k in range(n):
        needed = jnp.where(diagonal, h != k // half_n, side == k // half_n)

        @pl.when(jnp.logical_and(needed, me != k))
        def _():
            gathered(k).wait_recv()

    @pl.when(diagonal)
    def _():
        spare_rows().start()

    for s in range(len(order)):
        @pl.when(jnp.logical_not(wanted(peer(order[s]))))
        def _():
            gather(s).start()

    weight = jnp.where(diagonal, 1, 2).astype(jnp.float32)
    for t in range(2):
        lhs[t, :, :TILE] = (rows[:, tile_at(first[t])].astype(jnp.float32) * weight).astype(jnp.bfloat16)
        lhs[t, :, TILE:] = (rows[:, tile_at(second[t])].astype(jnp.float32) * 2.0).astype(jnp.bfloat16)

    @pl.when(relayed)
    def _():
        for j in range(half_n):
            arrived(j).wait_recv()
        for t in range(2):
            fj[t] = cols[:, t * TILE : (t + 1) * TILE].astype(jnp.float32)

    matrix_load.wait()
    total[...] = jnp.zeros_like(total)

    def add_moment(acc, prod, k):
        narrow = prod[:, :LANES] + prod[:, LANES:]
        return acc + jnp.sum(narrow, axis=-1, keepdims=True) * matrix[pl.ds(k, 1), :]

    def level_step(step, carry):
        acc = total[...]
        for u in range(UNROLL):
            k = step * UNROLL + u
            prod = None
            for t in range(2):
                image = jnp.dot(lhs[t], cheb[k, t], preferred_element_type=jnp.float32)
                term = image * fj[t]
                prod = term if prod is None else prod + term
            acc = add_moment(acc, prod, k)
        total[...] = acc
        return carry

    lax.fori_loop(0, LEVELS // UNROLL, level_step, 0)

    @pl.when(diagonal)
    def _():
        lhs_x[...] = (rows[:, tile_at(spare)].astype(jnp.float32) * 2.0).astype(jnp.bfloat16)

    @pl.when(helper)
    def _():
        spare_rows().wait_recv()
        lhs_x[...] = (rows_x[...].astype(jnp.float32) * 2.0).astype(jnp.bfloat16)

    @pl.when(jnp.logical_or(diagonal, helper))
    def _():
        base = jnp.where(diagonal, HALF, 0)

        def spare_step(step, carry):
            acc = total[...]
            for u in range(SPARE_UNROLL):
                k = step * SPARE_UNROLL + u
                image = jnp.dot(lhs_x[...], cheb_x[k], preferred_element_type=jnp.float32)
                acc = add_moment(acc, image * fj[h], base + k)
            total[...] = acc
            return carry

        lax.fori_loop(0, HALF // SPARE_UNROLL, spare_step, 0)

    share[...] = total[...].T[:L]

    chips = n_rows // 2
    piece = L // chips
    core, y = lax.rem(r, 2), r // 2

    def block(k):
        return pl.ds(pl.multiple_of(k * piece, piece), piece)

    def across(d):
        return lax.rem(y + d, chips)

    def reduce_line(d, source=core):
        k = across(d)
        return copy(
            share.at[block(k)], line_landed.at[2 * d + source], send4.at[d], recv4.at[2 * d + source],
            (2 * k + 1, c),
        )

    def exchange(s):
        return copy(line_sum, plane_landed.at[c], send5.at[s], recv5.at[s], (r, peer(order[s])))

    def spread_line(d, target, k):
        return copy(
            result, spectra_out.at[block(k)], send6.at[2 * d + target], recv6.at[d], (2 * across(d) + target, c)
        )

    def finish_rows():
        for k in range(n):
            needed = jnp.logical_or(diagonal, side == k // half_n)

            @pl.when(jnp.logical_and(jnp.logical_not(needed), me != k))
            def _():
                gathered(k).wait_recv()

    for d in (2, 3, 1):
        reduce_line(d).start()

    @pl.when(jnp.logical_not(lead))
    def _():
        reduce_line(0, 0).start()

    finish_rows()

    @pl.when(lead)
    def _():
        value = share[block(y)]
        for d, source in ((0, 0), (1, 0), (1, 1), (3, 0), (3, 1), (2, 0), (2, 1)):
            reduce_line(d, source).wait_recv()
            value = value + line_landed[2 * d + source]
        line_sum[...] = value
        for s in range(len(order)):
            exchange(s).start()
        plane_landed[c] = value
        for s in range(len(order)):
            exchange(s).wait_recv()
        value = plane_landed[0]
        for k in range(1, n):
            value = value + plane_landed[k]
        result[...] = value
        for d in (2, 3, 1):
            for target in range(2):
                spread_line(d, target, y).start()
        spread_line(0, 0, y).start()
        spectra_out[block(y)] = value

    for d in (1, 3, 2):
        spread_line(d, 0, lax.rem(y - d + chips, chips)).wait_recv()

    @pl.when(jnp.logical_not(lead))
    def _():
        spread_line(0, 0, y).wait_recv()
        reduce_line(0, 0).wait_send()

    for d in (1, 2, 3):
        reduce_line(d).wait_send()

    @pl.when(lead)
    def _():
        for s in range(len(order)):
            exchange(s).wait_send()
        for d in (1, 2, 3):
            for target in range(2):
                spread_line(d, target, y).wait_send()
        spread_line(0, 0, y).wait_send()

    @pl.when(relays)
    def _():
        for j in range(half_n):
            relay(j, place(cols, j)).wait_send()

    for s in range(len(order)):
        copy(parcel.at[0], landed.at[s], send1.at[s], recv1.at[s], (r, peer(order[s]))).wait_send()
        gather(s).wait_send()
    for e in SAME:
        column(e).wait_send()

    @pl.when(diagonal)
    def _():
        spare_cos().wait_send()
        spare_rows().wait_send()
        for j in range(half_n):
            @pl.when(me != h * half_n + j)
            def _():
                copy(rest.at[j], landed_rest, send_rest.at[j], recv_rest.at[0], (r, c)).wait_send()


def close_kernel(filtered, spectra, filtered_out, spectra_out, sem):
    copies = [
        pltpu.make_async_copy(filtered, filtered_out, sem.at[0]),
        pltpu.make_async_copy(spectra, spectra_out, sem.at[1]),
    ]
    for copy in copies:
        copy.start()
    for copy in copies:
        copy.wait()


def per_device(npix, n_rows, n_cols, inverse_cov, cosines, sky_maps):
    n_z = n_cols // N_X
    n = n_cols
    size, cols_here = inverse_cov.shape
    maps = sky_maps.shape[1]
    sky_t = sky_maps.T
    per, width = maps // 2, 2 * size // n
    piece = L // (n_rows // 2)
    vmem = pl.BlockSpec(memory_space=pltpu.VMEM)
    hbm = pl.BlockSpec(memory_space=pltpu.HBM)
    matrix = jnp.asarray(transform_matrix(npix))
    inputs = (sky_t, inverse_cov, cosines, matrix)
    bf16, f32 = jnp.bfloat16, jnp.float32
    plane = pltpu.SemaphoreType.DMA((n - 1,))
    line = pltpu.SemaphoreType.DMA((n_rows - 1,))
    half = pltpu.SemaphoreType.DMA((n // 2,))
    every = pltpu.SemaphoreType.DMA((n_rows,))
    filtered, spectra = pl.pallas_call(
        functools.partial(qml_kernel, n_rows, n_z, N_X),
        out_shape=(
            jax.ShapeDtypeStruct((maps, size), bf16),
            jax.ShapeDtypeStruct((L, maps), f32),
        ),
        in_specs=[hbm] * len(inputs),
        out_specs=(vmem, vmem),
        scratch_shapes=[
            pltpu.VMEM(sky_t.shape, bf16),
            pltpu.VMEM(inverse_cov.shape, bf16),
            pltpu.VMEM((5 * TILE, TILE), f32),
            pltpu.VMEM(matrix.shape, f32),
            pltpu.VMEM((LEVELS, 2, 2 * TILE, TILE), bf16),
            pltpu.VMEM((HALF, TILE, TILE), bf16),
            pltpu.VMEM((n, per, width), f32),
            pltpu.VMEM((n, per, width), bf16),
            pltpu.VMEM((n - 1, per, width), bf16),
            pltpu.VMEM((n // 2, per, width), bf16),
            pltpu.VMEM((per, width), bf16),
            pltpu.VMEM((per, width), bf16),
            pltpu.VMEM((maps, cols_here), bf16),
            pltpu.VMEM((2, maps, 2 * TILE), bf16),
            pltpu.VMEM((maps, TILE), bf16),
            pltpu.VMEM((maps, TILE), bf16),
            pltpu.VMEM((2, maps, TILE), f32),
            pltpu.VMEM((maps, LANES), f32),
            pltpu.VMEM((L, maps), f32),
            pltpu.VMEM((n_rows, piece, maps), f32),
            pltpu.VMEM((piece, maps), f32),
            pltpu.VMEM((n, piece, maps), f32),
            pltpu.VMEM((piece, maps), f32),
            pltpu.SemaphoreType.DMA((8,)),
            plane, pltpu.SemaphoreType.DMA((PARTS * (n - 1),)), half, pltpu.SemaphoreType.DMA((PARTS,)),
            plane, pltpu.SemaphoreType.DMA((n,)),
            line, half, line, every, plane, plane, every, line,
            pltpu.SemaphoreType.DMA((2,)), pltpu.SemaphoreType.DMA((2,)), half,
        ],
        compiler_params=pltpu.CompilerParams(
            collective_id=1, has_side_effects=True, vmem_limit_bytes=50 * 2**20
        ),
        name="qml",
    )(*[pltpu.with_memory_space_constraint(value, pltpu.HBM) for value in inputs])
    filtered, spectra = pl.pallas_call(
        close_kernel,
        out_shape=(pltpu.HBM(filtered.shape, bf16), pltpu.HBM(spectra.shape, f32)),
        in_specs=[vmem, vmem],
        out_specs=(hbm, hbm),
        scratch_shapes=[pltpu.SemaphoreType.DMA((2,))],
        compiler_params=pltpu.CompilerParams(vmem_limit_bytes=2**20),
        name="close",
    )(filtered, spectra)
    return filtered.T, spectra


def solution(mesh):
    in_specs = (P("prow", "pcol"), P("prow", "pcol"), P("pcol", None))
    out_specs = (P("prow", None), P())
    n_rows, n_cols = mesh.shape["prow"], mesh.shape["pcol"]

    def whole(inverse_cov, cosines, sky_maps):
        npix = cosines.shape[0]
        step = jax.shard_map(
            functools.partial(per_device, npix, n_rows, n_cols),
            mesh=mesh, in_specs=in_specs, out_specs=out_specs, check_vma=False,
        )
        return step(inverse_cov, cosines, sky_maps)

    return whole
```
